32 devices in a mesh: row: 4 (over x, core), col: 8 (over z, y).
Axes of the slice: x: 2, y: 2, z: 4, core: 2. Of those that a mesh axis runs over, the one named last changes fastest.
Arguments:
- rhs: float32 [4, 8, 8, 4, 128], P('row', 'col'), may hold values from -6 to 6
- diag0: float32 [4, 8, 8, 128], P('row', 'col'), may hold values from 2 to 4
- blocks0: float32 [4, 8, 8, 14, 128, 128], P('row', 'col'), may hold values from -0.1875 to 0.1875
- cols0: int32 [4, 8, 8, 14], P('row', 'col'), may hold values from 0 to 23
- sends0: int32 [4, 8, 4, 4], P('row', 'col'), may hold values from 0 to 7
- pro0: float32 [4, 8, 8, 128, 128], P('row', 'col'), may hold values from -0.5 to 0.5
- agg0: int32 [4, 8, 8], P('row', 'col'), may hold values from 0 to 1
- diag1: float32 [4, 8, 2, 128], P('row', 'col'), may hold values from 2 to 4
- blocks1: float32 [4, 8, 2, 14, 128, 128], P('row', 'col'), may hold values from -0.1875 to 0.1875
- cols1: int32 [4, 8, 2, 14], P('row', 'col'), may hold values from 0 to 9
- sends1: int32 [4, 8, 4, 2], P('row', 'col'), may hold values from 0 to 1
- pro1: float32 [4, 8, 2, 128, 128], P('row', 'col'), may hold values from -0.25 to 0.25
- agg1: int32 [4, 8, 2], P('row', 'col'), may hold values from 0 to 7
- cinv: float32 [1024, 1024], P(('row', 'col')), may hold values from -0.1875 to 0.1875
Outputs:
- solution: float32 [4, 8, 8, 4, 128], P('row', 'col')
The draws below stay inside these ranges and needn't reach their ends.
Inputs may be any that keep to these rules, and one draw needn't show every extreme that they name: `sends0`: indices of the sender's own fine blocks. `sends1`: indices of the sender's own level-one blocks. `cols0`: indices into the extended fine vector of 24 blocks. `cols1`: indices into the extended level-one vector of 10 blocks. `agg0`: a level-one block of the same partition. `agg1`: a coarsest block, on any partition.
All inputs are finite; a program needn't handle non-finite values.
Results may differ from the reference program's by a relative error of at most 0.0001.
Values sent between devices are 32-bit elements; how exact they have to be, the bound alone decides.
A program may use at most 64 MiB of HBM per device.

```python
import math
import jax
import jax.numpy as jnp
from jax import lax

BS = 128
NB = 8
NB1 = 2
K = 14
K1 = 14
G0 = 4
G1 = 2
NRHS = 4
NU = 2
NCB = 8
NCU = 1024
N_ROW = 4
N_COL = 8


def touch_ends(result, key, least, top_value):
    place = [jax.random.randint(jax.random.fold_in(key, axis), (), 0, length) for axis, length in enumerate(result.shape)]
    longest = result.shape.index(max(result.shape))
    next_to = place[:longest] + [(place[longest] + 1) % result.shape[longest]] + place[longest + 1:]
    return result.at[tuple(place)].set(least).at[tuple(next_to)].set(top_value)


def steps_of(stream_key, shape, shards, least, largest):
    gain = 1.0
    for dim, blocks in shards:
        steps = jax.random.uniform(jax.random.fold_in(jax.random.fold_in(stream_key, 6), dim), (blocks,), jnp.float32, least / len(shards), largest / len(shards))
        gain = gain * jnp.repeat(jnp.exp(steps), shape[dim] // blocks).reshape((-1,) + (1,) * (len(shape) - 1 - dim))
    return gain


def bell_draw(key, shape, spread, most, cuts=(), dtype=jnp.bfloat16):
    drawn = jax.random.normal(key, shape, jnp.float32) * spread
    if len(cuts) > 0:
        drawn = steps_of(key, shape, cuts, -0.22, 0.18) * drawn
    return jnp.clip(drawn, min=-most, max=most).astype(dtype)


def setup_inputs(seed: int = 0) -> dict:
    splits = jax.random.split(jax.random.key(seed), 15)
    rhs = bell_draw(splits[0], (N_ROW, N_COL, NB, NRHS, BS), 1.0, 6.0, ((0, 4), (1, 8)), jnp.float32)
    diag0 = jnp.clip(jnp.exp(math.log(4.0) - 0.6931472 * jax.random.uniform(splits[1], (N_ROW, N_COL, NB, BS), jnp.float32) ** steps_of(splits[1], (N_ROW, N_COL, NB, BS), ((0, 4), (1, 8)), -0.2, 0.2)), 2.0, 4.0)
    blocks0 = bell_draw(splits[2], (N_ROW, N_COL, NB, K, BS, BS), (K * BS // 2) ** -0.5, 0.1875, ((0, 4), (1, 8)), jnp.float32)
    cols0 = touch_ends(jax.random.randint(splits[3], (N_ROW, N_COL, NB, K), 0, NB + 4 * G0), jax.random.fold_in(splits[3], 1), 0, (NB + 4 * G0) - 1).astype(jnp.int32)
    sends0 = touch_ends(jax.random.randint(splits[4], (N_ROW, N_COL, 4, G0), 0, NB), jax.random.fold_in(splits[4], 1), 0, NB - 1).astype(jnp.int32)
    pro0 = bell_draw(splits[5], (N_ROW, N_COL, NB, BS, BS), BS ** -0.5, 0.5, ((0, 4), (1, 8)), jnp.float32)
    agg0 = touch_ends(jax.random.randint(splits[6], (N_ROW, N_COL, NB), 0, NB1), jax.random.fold_in(splits[6], 1), 0, NB1 - 1).astype(jnp.int32)
    diag1 = jnp.clip(jnp.exp(math.log(4.0) - 0.6931472 * jax.random.uniform(splits[7], (N_ROW, N_COL, NB1, BS), jnp.float32) ** steps_of(splits[7], (N_ROW, N_COL, NB1, BS), ((0, 4), (1, 8)), -0.2, 0.2)), 2.0, 4.0)
    blocks1 = bell_draw(splits[8], (N_ROW, N_COL, NB1, K1, BS, BS), (K1 * BS // 2) ** -0.5, 0.1875, ((0, 4), (1, 8)), jnp.float32)
    cols1 = touch_ends(jax.random.randint(splits[9], (N_ROW, N_COL, NB1, K1), 0, NB1 + 4 * G1), jax.random.fold_in(splits[9], 1), 0, (NB1 + 4 * G1) - 1).astype(jnp.int32)
    sends1 = touch_ends(jax.random.randint(splits[10], (N_ROW, N_COL, 4, G1), 0, NB1), jax.random.fold_in(splits[10], 1), 0, NB1 - 1).astype(jnp.int32)
    pro1 = bell_draw(splits[11], (N_ROW, N_COL, NB1, BS, BS), (4 * BS) ** -0.5, 0.25, ((0, 4), (1, 8)), jnp.float32)
    agg1 = touch_ends(jax.random.randint(splits[12], (N_ROW, N_COL, NB1), 0, NCB), jax.random.fold_in(splits[12], 1), 0, NCB - 1).astype(jnp.int32)
    cinv = bell_draw(splits[13], (NCU, NCU), NCU ** -0.5, 0.1875, ((0, 32),), jnp.float32)
    return dict(rhs=rhs, diag0=diag0, blocks0=blocks0, cols0=cols0, sends0=sends0, pro0=pro0, agg0=agg0, diag1=diag1, blocks1=blocks1, cols1=cols1, sends1=sends1, pro1=pro1, agg1=agg1, cinv=cinv)


HIGH = lax.Precision.HIGHEST
OMEGA = 0.3


def gather_ghosts(vector, sends):
    packed = jax.vmap(jax.vmap(lambda blocks, picks: blocks[picks]))(vector, sends)
    zero_row = jnp.zeros_like(packed[:1, :, 0])
    zero_col = jnp.zeros_like(packed[:, :1, 0])
    above = jnp.concatenate([zero_row, packed[:-1, :, 0]], axis=0)
    below = jnp.concatenate([packed[1:, :, 1], zero_row], axis=0)
    left = jnp.concatenate([zero_col, packed[:, :-1, 2]], axis=1)
    right = jnp.concatenate([packed[:, 1:, 3], zero_col], axis=1)
    return jnp.concatenate([vector, above, below, left, right], axis=2)


def apply_op(vector, diag, blocks, cols, sends):
    extended = gather_ghosts(vector, sends)
    nearby = jax.vmap(jax.vmap(lambda source, picks: source[picks]))(extended, cols)
    coupled = jnp.einsum('xybkij,xybkrj->xybri', blocks, nearby, precision=HIGH)
    return diag[..., None, :] * vector + coupled


def smooth(vector, right_side, diag, blocks, cols, sends, count):
    for sweep in range(count):
        vector = vector + OMEGA * (right_side - apply_op(vector, diag, blocks, cols, sends)) / diag[..., None, :]
    return vector


def reference(rhs, diag0, blocks0, cols0, sends0, pro0, agg0, diag1, blocks1, cols1, sends1, pro1, agg1, cinv):
    fine_x = OMEGA * rhs / diag0[..., None, :]
    fine_x = smooth(fine_x, rhs, diag0, blocks0, cols0, sends0, NU - 1)
    fine_res = rhs - apply_op(fine_x, diag0, blocks0, cols0, sends0)
    onehot0 = (agg0[..., None] == jnp.arange(NB1)).astype(jnp.float32)
    restricted = jnp.einsum('xybij,xybri->xybrj', pro0, fine_res, precision=HIGH)
    level_rhs = jnp.einsum('xybc,xybrj->xycrj', onehot0, restricted, precision=HIGH)
    level_x = OMEGA * level_rhs / diag1[..., None, :]
    level_x = smooth(level_x, level_rhs, diag1, blocks1, cols1, sends1, NU - 1)
    level_res = level_rhs - apply_op(level_x, diag1, blocks1, cols1, sends1)
    onehot1 = (agg1[..., None] == jnp.arange(NCB)).astype(jnp.float32)
    contrib = jnp.einsum('xybij,xybri->xybrj', pro1, level_res, precision=HIGH)
    coarse_rhs = jnp.einsum('xybc,xybrj->rcj', onehot1, contrib, precision=HIGH).reshape(NRHS, NCU)
    coarse_x = jnp.einsum('ij,rj->ri', cinv, coarse_rhs, precision=HIGH)
    coarse_blocks = coarse_x.reshape(NRHS, NCB, BS)
    picked = jnp.einsum('xybc,rcj->xybrj', onehot1, coarse_blocks, precision=HIGH)
    level_x = level_x + jnp.einsum('xybij,xybrj->xybri', pro1, picked, precision=HIGH)
    level_x = smooth(level_x, level_rhs, diag1, blocks1, cols1, sends1, NU)
    lifted = jnp.einsum('xybc,xycrj->xybrj', onehot0, level_x, precision=HIGH)
    fine_x = fine_x + jnp.einsum('xybij,xybrj->xybri', pro0, lifted, precision=HIGH)
    fine_x = smooth(fine_x, rhs, diag0, blocks0, cols0, sends0, NU)
    return fine_x
```

```python
import functools

import jax
import jax.numpy as jnp
from jax import lax
from jax.experimental import pallas as pl
from jax.experimental.pallas import tpu as pltpu
from jax.sharding import PartitionSpec as P

NU = 2
OMEGA = 0.3
F32 = jnp.float32
BF16 = jnp.bfloat16
MESH = pl.DeviceIdType.MESH
NN = (((1,), (0,)), ((), ()))


def two_terms(value):
    head = value.astype(BF16)
    tail = (value - head.astype(F32)).astype(BF16)
    return head, tail


def stacked(value):
    head = value.astype(BF16).astype(F32)
    rows = 2 * value.shape[0]
    pad = -rows % 16
    parts = [head, value - head]
    if pad:
        parts.append(jnp.zeros((pad, value.shape[1]), F32))
    return jnp.concatenate(parts, axis=0).astype(BF16)


def folded(lhs, wide):
    both = lax.dot_general(lhs, wide, NN, preferred_element_type=F32)
    half = both.shape[1] // 2
    return both[:, :half] + both[:, half:]


def joined(lhs, wide, rows):
    both = folded(lhs, wide)
    return both[:rows] + both[rows : 2 * rows]


def seat_of(group, groups, reps):
    if 2 * group + 1 < groups:
        return group * reps + reps - 1
    if 2 * group + 1 > groups:
        return group * reps
    return group * reps + reps // 2


def kernel(
    n_row, n_col, pair,
    cols0_h, sends0_h, agg0_h, cols1_h, sends1_h, agg1_h,
    rhs_h, diag0_h, blocks0_h, pro0_h, diag1_h, blocks1_h, pro1_h, cinv_h,
    out,
    rhs, diag0, blocks0, pro0, diag1, blocks1, pro1,
    cols0, sends0, agg0, cols1, sends1, agg1,
    in_sem,
    wide0, wide1, down0, up0, down1, up1, cin, wide2,
    dfull0, wfull0, dfull1, wfull1,
    ext0, ext1, x0, x1, b1, res0,
    send0, recv0, send1, recv1, psend, precv,
    aggf, recva, mine, recvc, xs, recvx, tally,
    s_send0, s_recv0, s_send1, s_recv1, s_psend, s_precv,
    s_cin, s_cown, s_csend, s_asend, s_msend, s_xsend, s_brecv,
):
    nb, loads, bs = rhs.shape
    nb1 = diag1.shape[0]
    k0 = blocks0.shape[1]
    k1 = blocks1.shape[1]
    g1 = send1.shape[2]
    n = n_row * n_col
    owned, ncu = cinv_h.shape
    ncb = ncu // bs
    reps = bs // owned
    groups = n_col // reps
    ns = (n_row // pair) * groups
    row = lax.axis_index("row")
    col = lax.axis_index("col")
    me = row * n_col + col

    seats = [seat_of(group, groups, reps) for group in range(groups)]
    solvers = [
        (tier * pair + pair - 1, seats[group])
        for tier in range(n_row // pair) for group in range(groups)
    ]
    my_tier, my_group = row // pair, col // reps
    my_seat = jnp.int32(0)
    for group in range(groups):
        my_seat = jnp.where(my_group == group, seats[group], my_seat)
    solving = (lax.rem(row, pair) == pair - 1) & (col == my_seat)
    my_place = my_tier * groups + my_group
    my_slot = lax.rem(row, pair) * reps + lax.rem(col, reps)

    directions = (
        (row < n_row - 1, (row + 1, col), row > 0),
        (row > 0, (row - 1, col), row < n_row - 1),
        (col < n_col - 1, (row, col + 1), col > 0),
        (col > 0, (row, col - 1), col < n_col - 1),
    )

    def wrapped(i, size):
        return jnp.where(i >= size, i - size, i)

    barrier = pltpu.get_barrier_semaphore()

    def greet(r, c):
        pl.semaphore_signal(barrier, inc=1, device_id=(r, c), device_id_type=MESH)

    loading = []

    def load(source, target):
        copy = pltpu.make_async_copy(source, target, in_sem.at[len(loading)])
        loading.append(copy)
        copy.start()
        return copy

    for i in range(1, n_row):
        greet(wrapped(row + i, n_row), col)
    l_ints = [
        load(source, target)
        for source, target in (
            (sends0_h, sends0), (cols0_h, cols0), (agg1_h, agg1),
            (agg0_h, agg0), (sends1_h, sends1), (cols1_h, cols1),
        )
    ]
    l_rhs = load(rhs_h, rhs)
    l_diag0 = load(diag0_h, diag0)
    l_blocks0 = [load(blocks0_h.at[b], blocks0.at[b]) for b in range(nb)]

    def greet_line(i, carry):
        c = wrapped(col + i, n_col)
        for r in range(n_row):
            greet(r, c)
        return carry

    lax.fori_loop(1, n_col, greet_line, 0, unroll=min(n_col - 1, 7))

    l_pro1 = load(pro1_h, pro1)
    l_pro0 = load(pro0_h, pro0)
    l_diag1 = load(diag1_h, diag1)
    l_blocks1 = load(blocks1_h, blocks1)

    for d, (_, _, comes) in enumerate(directions):
        @pl.when(jnp.logical_not(comes))
        def _():
            for e in range(recv0.shape[0]):
                recv0[e, d] = jnp.zeros(recv0.shape[2:], F32)
            for e in range(recv1.shape[0]):
                recv1[e, d] = jnp.zeros(recv1.shape[2:], F32)
            precv[d] = jnp.zeros(precv.shape[1:], F32)

    def halo_copy(send, recv, s_send, s_recv, e, d, there):
        return pltpu.make_async_remote_copy(
            src_ref=send.at[e, d], dst_ref=recv.at[e, d],
            send_sem=s_send.at[e, d], recv_sem=s_recv.at[e, d],
            device_id=there, device_id_type=MESH,
        )

    def pack(x, send, sends, e, flip=False):
        for d in range(4):
            for g in range(send.shape[2]):
                send[e, d, g] = x[sends[g, d] if flip else sends[d, g]]

    def start(send, recv, s_send, s_recv, e):
        for d in (2, 3, 0, 1):
            goes, there, _ = directions[d]

            @pl.when(goes)
            def _():
                halo_copy(send, recv, s_send, s_recv, e, d, there).start()

    def finish(send, recv, s_send, s_recv, e):
        with jax.named_scope("finish"):
            for d, (_, there, comes) in enumerate(directions):
                @pl.when(comes)
                def _():
                    halo_copy(send, recv, s_send, s_recv, e, d, (row, col)).wait_recv()

    def drain(send, recv, s_send, s_recv, e):
        for d, (goes, there, _) in enumerate(directions):
            @pl.when(goes)
            def _():
                halo_copy(send, recv, s_send, s_recv, e, d, there).wait_send()

    level0 = (send0, recv0, s_send0, s_recv0)
    level1 = (send1, recv1, s_send1, s_recv1)

    def bulk_copy(d, g, there):
        return pltpu.make_async_remote_copy(
            src_ref=psend.at[d, g], dst_ref=precv.at[d, g],
            send_sem=s_psend.at[d, g], recv_sem=s_precv.at[d, g],
            device_id=there, device_id_type=MESH,
        )

    def bulk_start(g):
        for d, (goes, there, _) in enumerate(directions):
            psend[d, g, :bs] = pro1[sends1[g, d]]
            psend[d, g, bs:] = jnp.full((8, bs), agg1[sends1[g, d]].astype(F32))

            @pl.when(goes)
            def _():
                bulk_copy(d, g, there).start()

    def own_ext(x, ext, count):
        for b in range(count):
            ext[b] = stacked(x[b])

    def ghost_ext(recv, ext, count, e):
        ghosts = recv.shape[2]
        for d in range(4):
            for g in range(ghosts):
                ext[count + d * ghosts + g] = stacked(recv[e, d, g])

    def coupled(b, cols, ext, wide, k):
        lhs = jnp.concatenate([ext[cols[b, i]] for i in range(k)], axis=1)
        return joined(lhs, wide[b], loads)

    def split_blocks(b, blocks, wide, k):
        def one(i, carry):
            h, t = two_terms(blocks[b, i].T)
            at = pl.ds(pl.multiple_of(i * bs, bs), bs)
            wide[b, at, :bs] = h
            wide[b, at, bs:] = t
            return carry

        lax.fori_loop(0, k, one, 0, unroll=7)

    def arrive(b):
        l_blocks0[b].wait()
        split_blocks(b, blocks0, wide0, k0)

    l_rhs.wait()
    l_diag0.wait()
    for b in range(nb):
        d = jnp.broadcast_to(diag0[b : b + 1, :], (loads, bs))
        w = OMEGA / d
        dfull0[b] = d
        wfull0[b] = w
        x0[b] = w * rhs[b]
    for copy in l_ints:
        copy.wait()
    pack(x0, send0, sends0, 0)
    for b in range(nb1):
        aggf[b * loads : (b + 1) * loads, :] = jnp.full((loads, bs), agg1[b].astype(F32))
    arrive(0)
    with jax.named_scope("barrier"):
        pl.semaphore_wait(barrier, n - 1)
    start(*level0, 0)

    def to_solvers(src, dst, s_send, which, wait=False):
        for i, (r, c) in enumerate(solvers):
            @pl.when((row != r) | (col != c))
            def _():
                copy = pltpu.make_async_remote_copy(
                    src_ref=src, dst_ref=dst.at[me],
                    send_sem=s_send.at[i], recv_sem=s_brecv.at[which],
                    device_id=(r, c), device_id_type=MESH,
                )
                if wait:
                    copy.wait_send()
                else:
                    copy.start()

    def all_bytes(dst, count, sem):
        part = dst.at[pl.ds(0, count)]
        pltpu.make_async_copy(part, part, sem).wait()

    def seat_copy(slot):
        return pltpu.make_async_remote_copy(
            src_ref=cinv_h, dst_ref=cin.at[slot],
            send_sem=s_csend.at[0], recv_sem=s_cin.at[slot],
            device_id=(my_tier * pair + pair - 1, my_seat), device_id_type=MESH,
        )

    own_rows = pltpu.make_async_copy(cinv_h, cin.at[my_slot], s_cown.at[0])

    @pl.when(solving)
    def _():
        own_rows.start()
        recva[me] = aggf[...]

    @pl.when(jnp.logical_not(solving))
    def _():
        seat_copy(my_slot).start()

    to_solvers(aggf, recva, s_asend, 0)
    own_ext(x0, ext0, nb)
    for b in range(1, nb):
        arrive(b)

    def sweep0(e, into):
        finish(*level0, e)
        with jax.named_scope("sweep0"):
            ghost_ext(recv0, ext0, nb, e)
            for b in range(nb):
                c = coupled(b, cols0, ext0, wide0, k0)
                v = x0[b]
                into[b] = v + wfull0[b] * (rhs[b] - (dfull0[b] * v + c))

    def sweep1(right, into):
        with jax.named_scope("sweep1"):
            for b in range(nb1):
                c = coupled(b, cols1, ext1, wide1, k1)
                v = x1[b]
                into[b] = v + wfull1[b] * (right[b] - (dfull1[b] * v + c))

    e0 = 0
    for _ in range(NU - 1):
        sweep0(e0, x0)
        e0 += 1
        pack(x0, send0, sends0, e0)
        start(*level0, e0)
        own_ext(x0, ext0, nb)

    l_pro1.wait()
    bulk_start(0)
    l_pro0.wait()
    for b in range(nb):
        h, t = two_terms(pro0[b])
        down0[b * bs : (b + 1) * bs, :bs] = h
        down0[b * bs : (b + 1) * bs, bs:] = t
    l_blocks1.wait()
    for b in range(nb1):
        split_blocks(b, blocks1, wide1, k1)
    l_diag1.wait()
    for b in range(nb1):
        d = jnp.broadcast_to(diag1[b : b + 1, :], (loads, bs))
        dfull1[b] = d
        wfull1[b] = OMEGA / d

    finish(*level0, e0)
    with jax.named_scope("resid0"):
        ghost_ext(recv0, ext0, nb, e0)
        for b in range(nb):
            c = coupled(b, cols0, ext0, wide0, k0)
            r = rhs[b] - (dfull0[b] * x0[b] + c)
            parts = [jnp.where(agg0[b] == a, r, 0.0) for a in range(nb1)]
            res0[:, b * bs : (b + 1) * bs] = stacked(jnp.concatenate(parts, axis=0))
        q = folded(res0[...], down0[...])
    e0 += 1

    for b in range(nb1):
        low = b * loads
        high = (nb1 + b) * loads
        total = q[low : low + loads] + q[high : high + loads]
        b1[b] = total
        x1[b] = wfull1[b] * total
    pack(x1, send1, sends1, 0, True)
    start(*level1, 0)
    own_ext(x1, ext1, nb1)
    for g in range(1, g1):
        bulk_start(g)
    for b in range(nb1):
        h, t = two_terms(pro1[b])
        down1[b, :, :bs] = h
        down1[b, :, bs:] = t
        h, t = two_terms(pro1[b].T)
        up1[b, :, :bs] = h
        up1[b, :, bs:] = t
    for b in range(nb):
        h, t = two_terms(pro0[b].T)
        up0[b, :, :bs] = h
        up0[b, :, bs:] = t
    e1 = 0
    for _ in range(NU - 1):
        finish(*level1, e1)
        ghost_ext(recv1, ext1, nb1, e1)
        sweep1(b1, x1)
        e1 += 1
        pack(x1, send1, sends1, e1, True)
        start(*level1, e1)
        own_ext(x1, ext1, nb1)

    @pl.when(solving)
    def _():
        own_rows.wait()
        for slot in range(pair * reps):
            @pl.when(my_slot != slot)
            def _():
                seat_copy(slot).wait_recv()

        def one(c, carry):
            at = pl.ds(pl.multiple_of(c * bs, bs), bs)
            for m in range(pair):
                piece = cin[m * reps : (m + 1) * reps, :, at].reshape(bs, bs)
                h, t = two_terms(piece.T)
                wide2[at, m * bs : (m + 1) * bs] = h
                wide2[at, (pair + m) * bs : (pair + m + 1) * bs] = t
            return carry

        lax.fori_loop(0, ncb, one, 0, unroll=4)

    finish(*level1, e1)
    with jax.named_scope("resid1"):
        ghost_ext(recv1, ext1, nb1, e1)
        for b in range(nb1):
            c = coupled(b, cols1, ext1, wide1, k1)
            r = b1[b] - (dfull1[b] * x1[b] + c)
            mine[b * loads : (b + 1) * loads, :] = joined(stacked(r), down1[b], loads)

    to_solvers(mine, recvc, s_msend, 1)

    @pl.when(solving)
    def _():
        recvc[me] = mine[...]

    for d, (_, _, comes) in enumerate(directions):
        for g in range(g1):
            @pl.when(comes)
            def _():
                bulk_copy(d, g, (row, col)).wait_recv()

            h, t = two_terms(precv[d, g, :bs].T)
            up1[nb1 + d * g1 + g, :, :bs] = h
            up1[nb1 + d * g1 + g, :, bs:] = t

    @pl.when(solving)
    def _():
        with jax.named_scope("waitC1"):
            all_bytes(recva, n - 1, s_brecv.at[0])
            all_bytes(recvc, n - 1, s_brecv.at[1])
        index = lax.broadcasted_iota(jnp.int32, (ncb, nb1 * loads, bs), 0).astype(F32)

        def collect(d, total):
            return total + jnp.where(recva[d][None] == index, recvc[d][None], 0.0)

        total = lax.fori_loop(
            0, n, collect, jnp.zeros((ncb, nb1 * loads, bs), F32), unroll=8
        )
        lhs = jnp.concatenate([stacked(total[c]) for c in range(ncb)], axis=1)
        own = folded(lhs, wide2[...])
        rows = [own[i * loads : (i + 1) * loads] for i in range(2 * nb1)]
        own = functools.reduce(lambda a, b: a + b, rows)
        for m in range(pair):
            xs[m] = own[:, m * bs : (m + 1) * bs]

        def tell(r, c):
            pltpu.make_async_remote_copy(
                src_ref=xs, dst_ref=recvx.at[my_place],
                send_sem=s_xsend.at[0], recv_sem=s_brecv.at[2],
                device_id=(r, c), device_id_type=MESH,
            ).start()

        half = n_col // 2
        for i in range(1, n_col):
            step = half + (i // 2 if i % 2 else -(i // 2))
            c = wrapped(col + step, n_col)
            for j in range(n_row):
                tell(wrapped(row + (j + 1) % n_row, n_row), c)
        for j in range(1, n_row):
            tell(wrapped(row + j, n_row), col)
        recvx[my_place] = xs[...]
        with jax.named_scope("waitC2"):
            if ns > 1:
                all_bytes(recvx, ns - 1, s_brecv.at[2])

    @pl.when(jnp.logical_not(solving))
    def _():
        with jax.named_scope("waitC2"):
            all_bytes(recvx, ns, s_brecv.at[2])

    names = [aggf[b * loads : (b + 1) * loads] for b in range(nb1)]
    names += [precv[d, g, bs : bs + loads] for d in range(4) for g in range(g1)]
    names = jnp.stack(names)

    def pick(tier, pieces):
        for m in range(pair):
            for group in range(groups):
                at = ((tier * pair + m) * groups + group).astype(F32)
                block = recvx[tier * groups + group, m]
                pieces = pieces + jnp.where(names == at, block[None], 0.0)
        return pieces

    pieces = lax.fori_loop(0, n_row // pair, pick, jnp.zeros(names.shape, F32), unroll=2)
    for b in range(nb1):
        x1[b] = x1[b] + joined(stacked(pieces[b]), up1[b], loads)
    for d in range(4):
        for g in range(g1):
            v = nb1 + d * g1 + g
            ghost = recv1[e1, d, g] + joined(stacked(pieces[v]), up1[v], loads)
            ext1[v] = stacked(ghost)
    e1 += 1

    for i in range(NU):
        own_ext(x1, ext1, nb1)
        if i > 0:
            finish(*level1, e1)
            ghost_ext(recv1, ext1, nb1, e1)
            e1 += 1
        sweep1(b1, x1)
        if i < NU - 1:
            pack(x1, send1, sends1, e1, True)
            start(*level1, e1)

    own_ext(x1, ext1, nb1)
    for b in range(nb):
        x0[b] = x0[b] + joined(ext1[agg0[b]], up0[b], loads)
    for i in range(NU):
        pack(x0, send0, sends0, e0)
        start(*level0, e0)
        own_ext(x0, ext0, nb)
        sweep0(e0, out if i == NU - 1 else x0)
        e0 += 1

    for e in range(e0):
        drain(*level0, e)
    for e in range(e1):
        drain(*level1, e)
    for d, (goes, there, _) in enumerate(directions):
        for g in range(g1):
            @pl.when(goes)
            def _():
                bulk_copy(d, g, there).wait_send()

    @pl.when(jnp.logical_not(solving))
    def _():
        seat_copy(my_slot).wait_send()

    @pl.when(solving)
    def _():
        all_bytes(tally, n - 1, s_xsend.at[0])

    to_solvers(aggf, recva, s_asend, 0, wait=True)
    to_solvers(mine, recvc, s_msend, 1, wait=True)


def on_device(
    rhs, diag0, blocks0, cols0, sends0, pro0, agg0, diag1, blocks1, cols1, sends1, pro1, agg1, cinv
):
    n_row, n_col = lax.axis_size("row"), lax.axis_size("col")
    n = n_row * n_col
    _, _, nb, loads, bs = rhs.shape
    nb1 = diag1.shape[2]
    k0, k1 = cols0.shape[3], cols1.shape[3]
    g0, g1 = sends0.shape[3], sends1.shape[3]
    owned, ncu = cinv.shape
    reps = bs // owned
    pair = 2 if n_row % 2 == 0 else 1
    ns = (n_row // pair) * (n_col // reps)
    tall = -(-2 * loads // 16) * 16
    floats = [a[0, 0] for a in (rhs, diag0, blocks0, pro0, diag1, blocks1, pro1)]
    ints = [a[0, 0] for a in (cols0, sends0, agg0, cols1)]
    ints += [sends1[0, 0].T, agg1[0, 0]]
    vm = pltpu.VMEM
    dma = pltpu.SemaphoreType.DMA
    scratch = [vm(a.shape, F32) for a in floats]
    scratch += [pltpu.SMEM(a.shape, jnp.int32) for a in ints]
    scratch += [dma((nb + 6 + len(ints),))]
    scratch += [vm((nb, k0 * bs, 2 * bs), BF16), vm((nb1, k1 * bs, 2 * bs), BF16)]
    scratch += [vm((nb * bs, 2 * bs), BF16), vm((nb, bs, 2 * bs), BF16)]
    scratch += [vm((nb1, bs, 2 * bs), BF16), vm((nb1 + 4 * g1, bs, 2 * bs), BF16)]
    scratch += [vm((pair * reps, owned, ncu), F32), vm((ncu, 2 * pair * bs), BF16)]
    scratch += [vm((nb, loads, bs), F32)] * 2
    scratch += [vm((nb1, loads, bs), F32)] * 2
    scratch += [vm((nb + 4 * g0, tall, bs), BF16), vm((nb1 + 4 * g1, tall, bs), BF16)]
    scratch += [vm((nb, loads, bs), F32), vm((nb1, loads, bs), F32), vm((nb1, loads, bs), F32)]
    scratch += [vm((-(-2 * nb1 * loads // 16) * 16, nb * bs), BF16)]
    scratch += [vm((2 * NU, 4, g0, loads, bs), F32)] * 2
    scratch += [vm((2 * NU - 1, 4, g1, loads, bs), F32)] * 2
    scratch += [vm((4, g1, bs + 8, bs), F32)] * 2
    scratch += [vm((nb1 * loads, bs), F32), vm((n, nb1 * loads, bs), F32)]
    scratch += [vm((nb1 * loads, bs), F32), vm((n, nb1 * loads, bs), F32)]
    scratch += [vm((pair, loads, bs), F32), vm((ns, pair, loads, bs), F32)]
    scratch += [vm((n - 1, pair, loads, bs), F32)]
    scratch += [dma((2 * NU, 4))] * 2 + [dma((2 * NU - 1, 4))] * 2 + [dma((4, g1))] * 2
    scratch += [dma((pair * reps,)), dma((1,)), dma((1,))]
    scratch += [dma((ns,))] * 2 + [dma((1,)), dma((3,))]
    result = pl.pallas_call(
        functools.partial(kernel, n_row, n_col, pair),
        out_shape=jax.ShapeDtypeStruct((nb, loads, bs), F32),
        in_specs=[pl.BlockSpec(memory_space=pl.ANY)] * 14,
        out_specs=pl.BlockSpec(memory_space=pltpu.VMEM),
        scratch_shapes=scratch,
        compiler_params=pltpu.CompilerParams(
            collective_id=0, has_side_effects=True, vmem_limit_bytes=60 * 1024 * 1024
        ),
    )(*ints, *floats, cinv)
    return result[None, None]


def solution(mesh):
    return jax.shard_map(
        on_device,
        mesh=mesh,
        in_specs=(
            P("row", "col", None, None, None),
            P("row", "col", None, None),
            P("row", "col", None, None, None, None),
            P("row", "col", None, None),
            P("row", "col", None, None),
            P("row", "col", None, None, None),
            P("row", "col", None),
            P("row", "col", None, None),
            P("row", "col", None, None, None, None),
            P("row", "col", None, None),
            P("row", "col", None, None),
            P("row", "col", None, None, None),
            P("row", "col", None),
            P(("row", "col"), None),
        ),
        out_specs=P("row", "col", None, None, None),
        check_vma=False,
    )
```

```python
import functools

import jax
import jax.numpy as jnp
from jax import lax
from jax.experimental import pallas as pl
from jax.experimental.pallas import tpu as pltpu
from jax.sharding import PartitionSpec as P

NU = 2
OMEGA = 0.3
F32 = jnp.float32
BF16 = jnp.bfloat16
MESH = pl.DeviceIdType.MESH
NN = (((1,), (0,)), ((), ()))


def two_terms(value):
    head = value.astype(BF16)
    tail = (value - head.astype(F32)).astype(BF16)
    return head, tail


def stacked(value):
    head = value.astype(BF16).astype(F32)
    rows = 2 * value.shape[0]
    pad = -rows % 16
    parts = [head, value - head]
    if pad:
        parts.append(jnp.zeros((pad, value.shape[1]), F32))
    return jnp.concatenate(parts, axis=0).astype(BF16)


def folded(lhs, wide):
    both = lax.dot_general(lhs, wide, NN, preferred_element_type=F32)
    half = both.shape[1] // 2
    return both[:, :half] + both[:, half:]


def joined(lhs, wide, rows):
    both = folded(lhs, wide)
    return both[:rows] + both[rows : 2 * rows]


def seat_of(group, groups, reps):
    if 2 * group + 1 < groups:
        return group * reps + reps - 1
    if 2 * group + 1 > groups:
        return group * reps
    return group * reps + reps // 2


def kernel(
    n_row, n_col, pair,
    cols0_h, sends0_h, agg0_h, cols1_h, sends1_h, agg1_h,
    rhs_h, diag0_h, blocks0_h, pro0_h, diag1_h, blocks1_h, pro1_h, cinv_h,
    out,
    rhs, diag0, blocks0, pro0, diag1, blocks1, pro1, cinv,
    cols0, sends0, agg0, cols1, sends1, agg1,
    in_sem,
    wide0, wide1, folded1, down0, up0, down1, up1, cin, wide2,
    dfull0, wfull0, dfull1, wfull1,
    ext0, ext1, x0, x1, b1, res0,
    send0, recv0, send1, recv1, psend, precv,
    aggf, recva, mine, recvc, xs, recvx, tally,
    s_send0, s_recv0, s_send1, s_recv1, s_psend, s_precv,
    s_cin, s_csend, s_asend, s_msend, s_xsend, s_brecv,
):
    nb, loads, bs = rhs.shape
    nb1 = diag1.shape[0]
    k0 = blocks0.shape[1]
    k1 = blocks1.shape[1]
    g1 = send1.shape[2]
    n = n_row * n_col
    owned, ncu = cinv.shape
    ncb = ncu // bs
    reps = bs // owned
    groups = n_col // reps
    ns = (n_row // pair) * groups
    row = lax.axis_index("row")
    col = lax.axis_index("col")
    me = row * n_col + col

    seats = [seat_of(group, groups, reps) for group in range(groups)]
    solvers = [
        (tier * pair + pair - 1, seats[group])
        for tier in range(n_row // pair) for group in range(groups)
    ]
    my_tier, my_group = row // pair, col // reps
    my_seat = jnp.int32(0)
    for group in range(groups):
        my_seat = jnp.where(my_group == group, seats[group], my_seat)
    solving = (lax.rem(row, pair) == pair - 1) & (col == my_seat)
    my_place = my_tier * groups + my_group
    my_slot = lax.rem(row, pair) * reps + lax.rem(col, reps)

    directions = (
        (row < n_row - 1, (row + 1, col), row > 0),
        (row > 0, (row - 1, col), row < n_row - 1),
        (col < n_col - 1, (row, col + 1), col > 0),
        (col > 0, (row, col - 1), col < n_col - 1),
    )

    def wrapped(i, size):
        return jnp.where(i >= size, i - size, i)

    barrier = pltpu.get_barrier_semaphore()

    def greet(r, c):
        pl.semaphore_signal(barrier, inc=1, device_id=(r, c), device_id_type=MESH)

    loading = []

    def load(source, target):
        copy = pltpu.make_async_copy(source, target, in_sem.at[len(loading)])
        loading.append(copy)
        copy.start()
        return copy

    for i in range(1, n_row):
        greet(wrapped(row + i, n_row), col)
    l_ints = [
        load(source, target)
        for source, target in (
            (sends0_h, sends0), (cols0_h, cols0), (agg1_h, agg1),
            (agg0_h, agg0), (sends1_h, sends1), (cols1_h, cols1),
        )
    ]
    l_rhs = load(rhs_h, rhs)
    l_diag0 = load(diag0_h, diag0)
    l_cinv = load(cinv_h, cinv)
    l_blocks0 = [load(blocks0_h.at[b], blocks0.at[b]) for b in range(nb)]

    def greet_line(i, carry):
        c = wrapped(col + i, n_col)
        for r in range(n_row):
            greet(r, c)
        return carry

    lax.fori_loop(1, n_col, greet_line, 0, unroll=min(n_col - 1, 7))

    l_pro1 = load(pro1_h, pro1)
    l_pro0 = load(pro0_h, pro0)
    l_diag1 = load(diag1_h, diag1)
    l_blocks1 = load(blocks1_h, blocks1)

    for d, (_, _, comes) in enumerate(directions):
        @pl.when(jnp.logical_not(comes))
        def _():
            for e in range(recv0.shape[0]):
                recv0[e, d] = jnp.zeros(recv0.shape[2:], F32)
            for e in range(recv1.shape[0]):
                recv1[e, d] = jnp.zeros(recv1.shape[2:], F32)
            precv[d] = jnp.zeros(precv.shape[1:], F32)

    def halo_copy(send, recv, s_send, s_recv, e, d, there):
        return pltpu.make_async_remote_copy(
            src_ref=send.at[e, d], dst_ref=recv.at[e, d],
            send_sem=s_send.at[e, d], recv_sem=s_recv.at[e, d],
            device_id=there, device_id_type=MESH,
        )

    def pack(x, send, sends, e, flip=False):
        for d in range(4):
            for g in range(send.shape[2]):
                send[e, d, g] = x[sends[g, d] if flip else sends[d, g]]

    def start(send, recv, s_send, s_recv, e):
        for d in (2, 3, 0, 1):
            goes, there, _ = directions[d]

            @pl.when(goes)
            def _():
                halo_copy(send, recv, s_send, s_recv, e, d, there).start()

    def finish(send, recv, s_send, s_recv, e):
        with jax.named_scope("finish"):
            for d, (_, there, comes) in enumerate(directions):
                @pl.when(comes)
                def _():
                    halo_copy(send, recv, s_send, s_recv, e, d, (row, col)).wait_recv()

    def drain(send, recv, s_send, s_recv, e):
        for d, (goes, there, _) in enumerate(directions):
            @pl.when(goes)
            def _():
                halo_copy(send, recv, s_send, s_recv, e, d, there).wait_send()

    level0 = (send0, recv0, s_send0, s_recv0)
    level1 = (send1, recv1, s_send1, s_recv1)

    def bulk_copy(d, g, there):
        return pltpu.make_async_remote_copy(
            src_ref=psend.at[d, g], dst_ref=precv.at[d, g],
            send_sem=s_psend.at[d, g], recv_sem=s_precv.at[d, g],
            device_id=there, device_id_type=MESH,
        )

    def bulk_start(g):
        for d, (goes, there, _) in enumerate(directions):
            psend[d, g, :bs] = pro1[sends1[g, d]]
            psend[d, g, bs:] = jnp.full((8, bs), agg1[sends1[g, d]].astype(F32))

            @pl.when(goes)
            def _():
                bulk_copy(d, g, there).start()

    def own_ext(x, ext, count):
        for b in range(count):
            ext[b] = stacked(x[b])

    def ghost_ext(recv, ext, count, e):
        ghosts = recv.shape[2]
        for d in range(4):
            for g in range(ghosts):
                ext[count + d * ghosts + g] = stacked(recv[e, d, g])

    def coupled(b, cols, ext, wide, k):
        lhs = jnp.concatenate([ext[cols[b, i]] for i in range(k)], axis=1)
        return joined(lhs, wide[b], loads)

    def split_blocks(b, blocks, wide, k):
        def one(i, carry):
            h, t = two_terms(blocks[b, i].T)
            at = pl.ds(pl.multiple_of(i * bs, bs), bs)
            wide[b, at, :bs] = h
            wide[b, at, bs:] = t
            return carry

        lax.fori_loop(0, k, one, 0, unroll=7)

    def arrive(b):
        l_blocks0[b].wait()
        split_blocks(b, blocks0, wide0, k0)

    l_rhs.wait()
    l_diag0.wait()
    for b in range(nb):
        d = jnp.broadcast_to(diag0[b : b + 1, :], (loads, bs))
        w = OMEGA / d
        dfull0[b] = d
        wfull0[b] = w
        x0[b] = w * rhs[b]
    for copy in l_ints:
        copy.wait()
    pack(x0, send0, sends0, 0)
    for b in range(nb1):
        aggf[b * loads : (b + 1) * loads, :] = jnp.full((loads, bs), agg1[b].astype(F32))
    arrive(0)
    with jax.named_scope("barrier"):
        pl.semaphore_wait(barrier, n - 1)
    start(*level0, 0)

    def to_solvers(src, dst, s_send, which, wait=False):
        for i, (r, c) in enumerate(solvers):
            @pl.when((row != r) | (col != c))
            def _():
                copy = pltpu.make_async_remote_copy(
                    src_ref=src, dst_ref=dst.at[me],
                    send_sem=s_send.at[i], recv_sem=s_brecv.at[which],
                    device_id=(r, c), device_id_type=MESH,
                )
                if wait:
                    copy.wait_send()
                else:
                    copy.start()

    def all_bytes(dst, count, sem):
        part = dst.at[pl.ds(0, count)]
        pltpu.make_async_copy(part, part, sem).wait()

    shares = s_csend.shape[0]
    width = ncu // shares

    def seat_copy(slot, share):
        lanes = pl.ds(share * width, width)
        return pltpu.make_async_remote_copy(
            src_ref=cinv.at[:, lanes], dst_ref=cin.at[slot, :, lanes],
            send_sem=s_csend.at[share], recv_sem=s_cin.at[slot, share],
            device_id=(my_tier * pair + pair - 1, my_seat), device_id_type=MESH,
        )

    def seat_start(share):
        @pl.when(jnp.logical_not(solving))
        def _():
            seat_copy(my_slot, share).start()

    def seat_ready(share):
        for slot in range(pair * reps):
            @pl.when(my_slot != slot)
            def _():
                seat_copy(slot, share).wait_recv()

        def one(c, carry):
            at = pl.ds(pl.multiple_of(c * bs, bs), bs)
            for m in range(pair):
                piece = cin[m * reps : (m + 1) * reps, :, at].reshape(bs, bs)
                h, t = two_terms(piece.T)
                wide2[at, m * bs : (m + 1) * bs] = h
                wide2[at, (pair + m) * bs : (pair + m + 1) * bs] = t
            return carry

        first = share * (ncb // shares)
        lax.fori_loop(first, first + ncb // shares, one, 0, unroll=4 if ncb // shares % 4 == 0 else 1)

    l_cinv.wait()

    @pl.when(solving)
    def _():
        cin[my_slot] = cinv[...]
        recva[me] = aggf[...]

    seat_start(0)
    to_solvers(aggf, recva, s_asend, 0)
    own_ext(x0, ext0, nb)
    for b in range(1, nb):
        arrive(b)

    def sweep0(e, into):
        finish(*level0, e)
        with jax.named_scope("sweep0"):
            ghost_ext(recv0, ext0, nb, e)
            for b in range(nb):
                c = coupled(b, cols0, ext0, wide0, k0)
                v = x0[b]
                into[b] = v + wfull0[b] * (rhs[b] - (dfull0[b] * v + c))

    def sweep1(right, into):
        with jax.named_scope("sweep1"):
            for b in range(nb1):
                c = coupled(b, cols1, ext1, wide1, k1)
                v = x1[b]
                into[b] = v + wfull1[b] * (right[b] - (dfull1[b] * v + c))

    e0 = 0
    for _ in range(NU - 1):
        sweep0(e0, x0)
        e0 += 1
        pack(x0, send0, sends0, e0)
        start(*level0, e0)
        own_ext(x0, ext0, nb)

    l_pro1.wait()
    bulk_start(0)
    l_pro0.wait()
    for b in range(nb):
        h, t = two_terms(pro0[b])
        down0[b * bs : (b + 1) * bs, :bs] = h
        down0[b * bs : (b + 1) * bs, bs:] = t
    l_blocks1.wait()
    for b in range(nb1):
        split_blocks(b, blocks1, wide1, k1)
    l_diag1.wait()
    for b in range(nb1):
        d = jnp.broadcast_to(diag1[b : b + 1, :], (loads, bs))
        dfull1[b] = d
        wfull1[b] = OMEGA / d

    finish(*level0, e0)
    with jax.named_scope("resid0"):
        ghost_ext(recv0, ext0, nb, e0)
        for b in range(nb):
            c = coupled(b, cols0, ext0, wide0, k0)
            r = rhs[b] - (dfull0[b] * x0[b] + c)
            parts = [jnp.where(agg0[b] == a, r, 0.0) for a in range(nb1)]
            res0[:, b * bs : (b + 1) * bs] = stacked(jnp.concatenate(parts, axis=0))
        q = folded(res0[...], down0[...])
    e0 += 1

    for b in range(nb1):
        low = b * loads
        high = (nb1 + b) * loads
        total = q[low : low + loads] + q[high : high + loads]
        b1[b] = total
        x1[b] = wfull1[b] * total
    pack(x1, send1, sends1, 0, True)
    start(*level1, 0)
    own_ext(x1, ext1, nb1)
    for share in range(1, shares):
        seat_start(share)
    for b in range(nb1):
        h, t = two_terms(pro1[b])
        down1[b, :, :bs] = h
        down1[b, :, bs:] = t
        h, t = two_terms(pro1[b].T)
        up1[b, :, :bs] = h
        up1[b, :, bs:] = t
    for b in range(nb1):
        twice = jnp.concatenate([down1[b], down1[b]], axis=0)

        def fold(i, carry):
            at = pl.ds(pl.multiple_of(i * bs, bs), bs)
            h, t = two_terms(folded(wide1[b, at], twice))
            folded1[b, at, :bs] = h
            folded1[b, at, bs:] = t
            return carry

        lax.fori_loop(0, k1, fold, 0, unroll=7)
    for b in range(nb):
        h, t = two_terms(pro0[b].T)
        up0[b, :, :bs] = h
        up0[b, :, bs:] = t
    e1 = 0
    for _ in range(NU - 1):
        finish(*level1, e1)
        ghost_ext(recv1, ext1, nb1, e1)
        sweep1(b1, x1)
        e1 += 1
        pack(x1, send1, sends1, e1, True)
        start(*level1, e1)
        own_ext(x1, ext1, nb1)

    @pl.when(solving)
    def _():
        seat_ready(0)

    base = [
        joined(stacked(b1[b] - dfull1[b] * x1[b]), down1[b], loads) for b in range(nb1)
    ]
    finish(*level1, e1)
    with jax.named_scope("resid1"):
        ghost_ext(recv1, ext1, nb1, e1)
        for b in range(nb1):
            c = coupled(b, cols1, ext1, folded1, k1)
            mine[b * loads : (b + 1) * loads, :] = base[b] - c

    to_solvers(mine, recvc, s_msend, 1)

    @pl.when(solving)
    def _():
        recvc[me] = mine[...]

    for g in range(1, g1):
        bulk_start(g)

    @pl.when(solving)
    def _():
        for share in range(1, shares):
            seat_ready(share)
        with jax.named_scope("waitC1"):
            all_bytes(recva, n - 1, s_brecv.at[0])
            all_bytes(recvc, n - 1, s_brecv.at[1])
        index = lax.broadcasted_iota(jnp.int32, (ncb, nb1 * loads, bs), 0).astype(F32)

        def collect(d, total):
            return total + jnp.where(recva[d][None] == index, recvc[d][None], 0.0)

        total = lax.fori_loop(
            0, n, collect, jnp.zeros((ncb, nb1 * loads, bs), F32), unroll=8
        )
        lhs = jnp.concatenate([stacked(total[c]) for c in range(ncb)], axis=1)
        own = folded(lhs, wide2[...])
        rows = [own[i * loads : (i + 1) * loads] for i in range(2 * nb1)]
        own = functools.reduce(lambda a, b: a + b, rows)
        for m in range(pair):
            xs[m] = own[:, m * bs : (m + 1) * bs]

        def tell(r, c):
            pltpu.make_async_remote_copy(
                src_ref=xs, dst_ref=recvx.at[my_place],
                send_sem=s_xsend.at[0], recv_sem=s_brecv.at[2],
                device_id=(r, c), device_id_type=MESH,
            ).start()

        half = n_col // 2
        for i in range(1, n_col):
            step = half + (i // 2 if i % 2 else -(i // 2))
            c = wrapped(col + step, n_col)
            for j in range(n_row):
                tell(wrapped(row + (j + 1) % n_row, n_row), c)
        for j in range(1, n_row):
            tell(wrapped(row + j, n_row), col)
        recvx[my_place] = xs[...]

    for d, (_, _, comes) in enumerate(directions):
        for g in range(g1):
            @pl.when(comes)
            def _():
                bulk_copy(d, g, (row, col)).wait_recv()

            h, t = two_terms(precv[d, g, :bs].T)
            up1[nb1 + d * g1 + g, :, :bs] = h
            up1[nb1 + d * g1 + g, :, bs:] = t

    @pl.when(solving)
    def _():
        with jax.named_scope("waitC2"):
            if ns > 1:
                all_bytes(recvx, ns - 1, s_brecv.at[2])

    @pl.when(jnp.logical_not(solving))
    def _():
        with jax.named_scope("waitC2"):
            all_bytes(recvx, ns, s_brecv.at[2])

    names = [aggf[b * loads : (b + 1) * loads] for b in range(nb1)]
    names += [precv[d, g, bs : bs + loads] for d in range(4) for g in range(g1)]
    names = jnp.stack(names)

    def pick(tier, pieces):
        for m in range(pair):
            for group in range(groups):
                at = ((tier * pair + m) * groups + group).astype(F32)
                block = recvx[tier * groups + group, m]
                pieces = pieces + jnp.where(names == at, block[None], 0.0)
        return pieces

    pieces = lax.fori_loop(0, n_row // pair, pick, jnp.zeros(names.shape, F32), unroll=2)
    for b in range(nb1):
        x1[b] = x1[b] + joined(stacked(pieces[b]), up1[b], loads)
    for d in range(4):
        for g in range(g1):
            v = nb1 + d * g1 + g
            ghost = recv1[e1, d, g] + joined(stacked(pieces[v]), up1[v], loads)
            ext1[v] = stacked(ghost)
    e1 += 1

    for i in range(NU):
        own_ext(x1, ext1, nb1)
        if i > 0:
            finish(*level1, e1)
            ghost_ext(recv1, ext1, nb1, e1)
            e1 += 1
        sweep1(b1, x1)
        if i < NU - 1:
            pack(x1, send1, sends1, e1, True)
            start(*level1, e1)

    own_ext(x1, ext1, nb1)
    for b in range(nb):
        x0[b] = x0[b] + joined(ext1[agg0[b]], up0[b], loads)
    for i in range(NU):
        pack(x0, send0, sends0, e0)
        start(*level0, e0)
        own_ext(x0, ext0, nb)
        if i == NU - 1:
            for e in range(e0):
                drain(*level0, e)
            for e in range(e1):
                drain(*level1, e)
            for d, (goes, there, _) in enumerate(directions):
                for g in range(g1):
                    @pl.when(goes)
                    def _():
                        bulk_copy(d, g, there).wait_send()

            @pl.when(jnp.logical_not(solving))
            def _():
                for share in range(shares):
                    seat_copy(my_slot, share).wait_send()

            @pl.when(solving)
            def _():
                all_bytes(tally, n - 1, s_xsend.at[0])

            to_solvers(aggf, recva, s_asend, 0, wait=True)
            to_solvers(mine, recvc, s_msend, 1, wait=True)
        sweep0(e0, out if i == NU - 1 else x0)
        e0 += 1

    drain(*level0, e0 - 1)


def on_device(
    rhs, diag0, blocks0, cols0, sends0, pro0, agg0, diag1, blocks1, cols1, sends1, pro1, agg1, cinv
):
    n_row, n_col = lax.axis_size("row"), lax.axis_size("col")
    n = n_row * n_col
    _, _, nb, loads, bs = rhs.shape
    nb1 = diag1.shape[2]
    k0, k1 = cols0.shape[3], cols1.shape[3]
    g0, g1 = sends0.shape[3], sends1.shape[3]
    owned, ncu = cinv.shape
    reps = bs // owned
    pair = 2 if n_row % 2 == 0 else 1
    ns = (n_row // pair) * (n_col // reps)
    shares = 2 if (ncu // bs) % 2 == 0 else 1
    tall = -(-2 * loads // 16) * 16
    floats = [a[0, 0] for a in (rhs, diag0, blocks0, pro0, diag1, blocks1, pro1)] + [cinv]
    ints = [a[0, 0] for a in (cols0, sends0, agg0, cols1)]
    ints += [sends1[0, 0].T, agg1[0, 0]]
    vm = pltpu.VMEM
    dma = pltpu.SemaphoreType.DMA
    scratch = [vm(a.shape, F32) for a in floats]
    scratch += [pltpu.SMEM(a.shape, jnp.int32) for a in ints]
    scratch += [dma((nb + 7 + len(ints),))]
    scratch += [vm((nb, k0 * bs, 2 * bs), BF16)] + [vm((nb1, k1 * bs, 2 * bs), BF16)] * 2
    scratch += [vm((nb * bs, 2 * bs), BF16), vm((nb, bs, 2 * bs), BF16)]
    scratch += [vm((nb1, bs, 2 * bs), BF16), vm((nb1 + 4 * g1, bs, 2 * bs), BF16)]
    scratch += [vm((pair * reps, owned, ncu), F32), vm((ncu, 2 * pair * bs), BF16)]
    scratch += [vm((nb, loads, bs), F32)] * 2
    scratch += [vm((nb1, loads, bs), F32)] * 2
    scratch += [vm((nb + 4 * g0, tall, bs), BF16), vm((nb1 + 4 * g1, tall, bs), BF16)]
    scratch += [vm((nb, loads, bs), F32), vm((nb1, loads, bs), F32), vm((nb1, loads, bs), F32)]
    scratch += [vm((-(-2 * nb1 * loads // 16) * 16, nb * bs), BF16)]
    scratch += [vm((2 * NU, 4, g0, loads, bs), F32)] * 2
    scratch += [vm((2 * NU - 1, 4, g1, loads, bs), F32)] * 2
    scratch += [vm((4, g1, bs + 8, bs), F32)] * 2
    scratch += [vm((nb1 * loads, bs), F32), vm((n, nb1 * loads, bs), F32)]
    scratch += [vm((nb1 * loads, bs), F32), vm((n, nb1 * loads, bs), F32)]
    scratch += [vm((pair, loads, bs), F32), vm((ns, pair, loads, bs), F32)]
    scratch += [vm((n - 1, pair, loads, bs), F32)]
    scratch += [dma((2 * NU, 4))] * 2 + [dma((2 * NU - 1, 4))] * 2 + [dma((4, g1))] * 2
    scratch += [dma((pair * reps, shares)), dma((shares,))]
    scratch += [dma((ns,))] * 2 + [dma((1,)), dma((3,))]
    result = pl.pallas_call(
        functools.partial(kernel, n_row, n_col, pair),
        out_shape=pltpu.VMEM((nb, loads, bs), F32),
        in_specs=[pl.BlockSpec(memory_space=pl.ANY)] * 14,
        out_specs=pl.BlockSpec(memory_space=pltpu.VMEM),
        scratch_shapes=scratch,
        compiler_params=pltpu.CompilerParams(
            collective_id=0, has_side_effects=True, vmem_limit_bytes=60 * 1024 * 1024
        ),
    )(*ints, *floats)
    return result[None, None]


def solution(mesh):
    return jax.shard_map(
        on_device,
        mesh=mesh,
        in_specs=(
            P("row", "col", None, None, None),
            P("row", "col", None, None),
            P("row", "col", None, None, None, None),
            P("row", "col", None, None),
            P("row", "col", None, None),
            P("row", "col", None, None, None),
            P("row", "col", None),
            P("row", "col", None, None),
            P("row", "col", None, None, None, None),
            P("row", "col", None, None),
            P("row", "col", None, None),
            P("row", "col", None, None, None),
            P("row", "col", None),
            P(("row", "col"), None),
        ),
        out_specs=P("row", "col", None, None, None),
        check_vma=False,
    )
```

```python
import functools

import jax
import jax.numpy as jnp
from jax import lax
from jax.experimental import pallas as pl
from jax.experimental.pallas import tpu as pltpu
from jax.sharding import PartitionSpec as P

NU = 2
OMEGA = 0.3
F32 = jnp.float32
BF16 = jnp.bfloat16
MESH = pl.DeviceIdType.MESH
NN = (((1,), (0,)), ((), ()))


def two_terms(value):
    head = value.astype(BF16)
    tail = (value - head.astype(F32)).astype(BF16)
    return head, tail


def stacked(value):
    head = value.astype(BF16).astype(F32)
    rows = 2 * value.shape[0]
    pad = -rows % 16
    parts = [head, value - head]
    if pad:
        parts.append(jnp.zeros((pad, value.shape[1]), F32))
    return jnp.concatenate(parts, axis=0).astype(BF16)


def folded(lhs, wide):
    both = lax.dot_general(lhs, wide, NN, preferred_element_type=F32)
    half = both.shape[1] // 2
    return both[:, :half] + both[:, half:]


def joined(lhs, wide, rows):
    both = folded(lhs, wide)
    return both[:rows] + both[rows : 2 * rows]


def seat_of(group, groups, reps):
    if 2 * group + 1 < groups:
        return group * reps + reps - 1
    if 2 * group + 1 > groups:
        return group * reps
    return group * reps + reps // 2


def reaches(n_row, n_col, pair, groups, reps):
    grid = [(r, c) for r in range(n_row) for c in range(n_col)]

    def beside(p, row_steps, col_steps):
        steps = [(d, 0) for d in row_steps] + [(0, d) for d in col_steps]
        spots = [(p[0] + a, p[1] + b) for a, b in steps]
        return [q for q in spots if 0 <= q[0] < n_row and 0 <= q[1] < n_col]

    def heard(known, jump):
        told = {}
        for p in grid:
            near = beside(p, (-1, 1), (-1, 1)) + (beside(p, (), (-2, 2)) if jump else [])
            told[p] = known[p].union(*[known[q] for q in near])
        return told

    first = heard({p: {p} for p in grid}, False)
    second = heard(first, False)
    third = heard(second, True)
    last = heard(heard(third, True), False)
    seats = [seat_of(group, groups, reps) for group in range(groups)]
    for r, c in grid:
        own = (r // pair * pair + pair - 1, seats[c // reps])
        solvers = {(t, s) for t in range(pair - 1, n_row, pair) for s in seats}
        if own not in third[(r, c)] or not solvers <= last[(r, c)]:
            return False
    return True


def kernel(
    n_row, n_col, pair,
    cols0_h, sends0_h, agg0_h, cols1_h, sends1_h, agg1_h,
    rhs_h, diag0_h, blocks0_h, pro0_h, diag1_h, blocks1_h, pro1_h, cinv_h,
    out,
    rhs, diag0, blocks0, pro0, diag1, blocks1, pro1, cinv,
    cols0, sends0, agg0, cols1, sends1, agg1,
    in_sem,
    wide0, wide1, folded1, down0, up0, down1, up1, cin, wide2,
    dfull0, wfull0, dfull1, wfull1,
    ext0, ext1, x0, x1, b1, res0,
    send0, recv0, send1, recv1, psend, precv,
    aggf, recva, mine, recvc, xs, recvx, tally,
    s_send, s_recv, s_psend, s_precv,
    s_cin, s_csend, s_asend, s_msend, s_xsend, s_brecv, s_far,
):
    nb, loads, bs = rhs.shape
    nb1 = diag1.shape[0]
    k0 = blocks0.shape[1]
    k1 = blocks1.shape[1]
    g1 = send1.shape[2]
    n = n_row * n_col
    owned, ncu = cinv.shape
    ncb = ncu // bs
    reps = bs // owned
    groups = n_col // reps
    ns = (n_row // pair) * groups
    row = lax.axis_index("row")
    col = lax.axis_index("col")
    me = row * n_col + col

    seats = [seat_of(group, groups, reps) for group in range(groups)]
    solvers = [
        (tier * pair + pair - 1, seats[group])
        for tier in range(n_row // pair) for group in range(groups)
    ]
    my_tier, my_group = row // pair, col // reps
    my_seat = jnp.int32(0)
    for group in range(groups):
        my_seat = jnp.where(my_group == group, seats[group], my_seat)
    solving = (lax.rem(row, pair) == pair - 1) & (col == my_seat)
    my_place = my_tier * groups + my_group
    my_slot = lax.rem(row, pair) * reps + lax.rem(col, reps)

    directions = (
        (row < n_row - 1, (row + 1, col), row > 0),
        (row > 0, (row - 1, col), row < n_row - 1),
        (col < n_col - 1, (row, col + 1), col > 0),
        (col > 0, (row, col - 1), col < n_col - 1),
    )

    def wrapped(i, size):
        return jnp.where(i >= size, i - size, i)

    barrier = pltpu.get_barrier_semaphore()
    relayed = reaches(n_row, n_col, pair, groups, reps)

    def greet(r, c):
        pl.semaphore_signal(barrier, inc=1, device_id=(r, c), device_id_type=MESH)

    loading = []

    def load(source, target):
        copy = pltpu.make_async_copy(source, target, in_sem.at[len(loading) % in_sem.shape[0]])
        loading.append(copy)
        copy.start()
        return copy

    if relayed:
        for goes, (r, c), _ in directions:
            @pl.when(goes)
            def _():
                greet(r, c)
    else:
        for i in range(1, n_row):
            greet(wrapped(row + i, n_row), col)

    l_ints = [
        load(source, target)
        for source, target in (
            (sends0_h, sends0), (sends1_h, sends1), (agg1_h, agg1),
            (agg0_h, agg0), (cols0_h, cols0), (cols1_h, cols1),
        )
    ]
    l_rhs = load(rhs_h, rhs)
    l_diag0 = load(diag0_h, diag0)
    l_pro1 = load(pro1_h, pro1)
    l_blocks0 = [load(blocks0_h.at[b], blocks0.at[b]) for b in range(nb)]

    if not relayed:
        def greet_line(i, carry):
            c = wrapped(col + i, n_col)
            for r in range(n_row):
                greet(r, c)
            return carry

        lax.fori_loop(1, n_col, greet_line, 0, unroll=min(n_col - 1, 7))

    for d, (_, _, comes) in enumerate(directions):
        @pl.when(jnp.logical_not(comes))
        def _():
            for e in range(recv0.shape[0]):
                recv0[e, d] = jnp.zeros(recv0.shape[2:], F32)
            for e in range(recv1.shape[0]):
                recv1[e, d] = jnp.zeros(recv1.shape[2:], F32)
            precv[d] = jnp.zeros(precv.shape[1:], F32)

    order = []

    def halo_copy(level, e, d, there):
        send, recv = level
        turn = order.index((level is level1, e)) % 2
        return pltpu.make_async_remote_copy(
            src_ref=send.at[e, d], dst_ref=recv.at[e, d],
            send_sem=s_send.at[turn, d], recv_sem=s_recv.at[turn, d],
            device_id=there, device_id_type=MESH,
        )

    def pack(x, send, sends, e, flip=False):
        for d in range(4):
            for g in range(send.shape[2]):
                send[e, d, g] = x[sends[g, d] if flip else sends[d, g]]

    def start(level, e):
        order.append((level is level1, e))
        for d in (2, 3, 0, 1):
            goes, there, _ = directions[d]

            @pl.when(goes)
            def _():
                halo_copy(level, e, d, there).start()

    def finish(level, e):
        with jax.named_scope("finish"):
            for d, (_, there, comes) in enumerate(directions):
                @pl.when(comes)
                def _():
                    halo_copy(level, e, d, (row, col)).wait_recv()

    def drain(back):
        if back > len(order):
            return
        upper, e = order[-back]
        for d, (goes, there, _) in enumerate(directions):
            @pl.when(goes)
            def _():
                halo_copy(level1 if upper else level0, e, d, there).wait_send()

    level0 = (send0, recv0)
    level1 = (send1, recv1)

    def bulk_copy(d, g, there):
        return pltpu.make_async_remote_copy(
            src_ref=psend.at[d, g], dst_ref=precv.at[d, g],
            send_sem=s_psend.at[d, g], recv_sem=s_precv.at[d, g],
            device_id=there, device_id_type=MESH,
        )

    def bulk_start(g):
        for d, (goes, there, _) in enumerate(directions):
            psend[d, g, :bs] = pro1[sends1[g, d]]
            psend[d, g, bs:] = jnp.full((8, bs), agg1[sends1[g, d]].astype(F32))

            @pl.when(goes)
            def _():
                bulk_copy(d, g, there).start()

    def own_ext(x, ext, count):
        for b in range(count):
            ext[b] = stacked(x[b])

    def ghost_ext(recv, ext, count, e):
        ghosts = recv.shape[2]
        for d in range(4):
            for g in range(ghosts):
                ext[count + d * ghosts + g] = stacked(recv[e, d, g])

    def coupled(b, cols, ext, wide, k):
        lhs = jnp.concatenate([ext[cols[b, i]] for i in range(k)], axis=1)
        return joined(lhs, wide[b], loads)

    def split_blocks(b, blocks, wide, k):
        def one(i, carry):
            h, t = two_terms(blocks[b, i].T)
            at = pl.ds(pl.multiple_of(i * bs, bs), bs)
            wide[b, at, :bs] = h
            wide[b, at, bs:] = t
            return carry

        lax.fori_loop(0, k, one, 0, unroll=7)

    def arrive(b):
        l_blocks0[b].wait()
        split_blocks(b, blocks0, wide0, k0)

    l_rhs.wait()
    l_diag0.wait()
    for b in range(nb):
        d = jnp.broadcast_to(diag0[b : b + 1, :], (loads, bs))
        w = OMEGA / d
        dfull0[b] = d
        wfull0[b] = w
        x0[b] = w * rhs[b]
    for copy in l_ints:
        copy.wait()
    pack(x0, send0, sends0, 0)
    with jax.named_scope("barrier"):
        if relayed:
            count = jnp.int32(0)
            for _, _, comes in directions:
                count = count + jnp.where(comes, 1, 0)
            pl.semaphore_wait(barrier, count)
        else:
            pl.semaphore_wait(barrier, n - 1)
    start(level0, 0)
    l_pro1.wait()
    bulk_start(0)
    l_cinv = load(cinv_h, cinv)
    l_pro0 = load(pro0_h, pro0)
    l_diag1 = load(diag1_h, diag1)
    l_blocks1 = load(blocks1_h, blocks1)
    own_ext(x0, ext0, nb)
    for b in range(nb1):
        aggf[b : b + 1, :] = jnp.full((1, bs), agg1[b].astype(F32))
    for b in range(nb):
        arrive(b)

    def tell_far(jump):
        if relayed:
            for goes, c in ((col + 2 < n_col, col + 2), (col > 1, col - 2)):
                @pl.when(goes)
                def _():
                    pl.semaphore_signal(
                        s_far.at[jump], inc=1, device_id=(row, c), device_id_type=MESH
                    )

    def hear_far(jump):
        if relayed:
            count = jnp.where(col + 2 < n_col, 1, 0) + jnp.where(col > 1, 1, 0)
            pl.semaphore_wait(s_far.at[jump], count)

    def to_solvers(src, dst, s_out, which):
        for r, c in solvers:
            @pl.when((row != r) | (col != c))
            def _():
                pltpu.make_async_remote_copy(
                    src_ref=src, dst_ref=dst.at[me],
                    send_sem=s_out.at[0], recv_sem=s_brecv.at[which],
                    device_id=(r, c), device_id_type=MESH,
                ).start()

    def all_bytes(dst, count, sem):
        part = dst.at[pl.ds(0, count)]
        pltpu.make_async_copy(part, part, sem).wait()

    shares = s_csend.shape[0]
    width = ncu // shares

    def seat_copy(slot, share):
        lanes = pl.ds(share * width, width)
        return pltpu.make_async_remote_copy(
            src_ref=cinv.at[:, lanes], dst_ref=cin.at[slot, :, lanes],
            send_sem=s_csend.at[share], recv_sem=s_cin.at[share],
            device_id=(my_tier * pair + pair - 1, my_seat), device_id_type=MESH,
        )

    def seat_start(share):
        @pl.when(jnp.logical_not(solving))
        def _():
            seat_copy(my_slot, share).start()

    def seat_ready(share):
        if pair * reps > 1:
            part = cin.at[pl.ds(0, pair * reps - 1), :, pl.ds(share * width, width)]
            pltpu.make_async_copy(part, part, s_cin.at[share]).wait()

        def one(c, carry):
            at = pl.ds(pl.multiple_of(c * bs, bs), bs)
            for m in range(pair):
                piece = cin[m * reps : (m + 1) * reps, :, at].reshape(bs, bs)
                h, t = two_terms(piece.T)
                wide2[at, m * bs : (m + 1) * bs] = h
                wide2[at, (pair + m) * bs : (pair + m + 1) * bs] = t
            return carry

        first = share * (ncb // shares)
        lax.fori_loop(first, first + ncb // shares, one, 0, unroll=4 if ncb // shares % 4 == 0 else 1)

    def sweep0(e, into):
        finish(level0, e)
        if e == 0:
            tell_far(0)
        with jax.named_scope("sweep0"):
            ghost_ext(recv0, ext0, nb, e)
            for b in range(nb):
                c = coupled(b, cols0, ext0, wide0, k0)
                v = x0[b]
                into[b] = v + wfull0[b] * (rhs[b] - (dfull0[b] * v + c))

    def sweep1(right, into):
        with jax.named_scope("sweep1"):
            for b in range(nb1):
                c = coupled(b, cols1, ext1, wide1, k1)
                v = x1[b]
                into[b] = v + wfull1[b] * (right[b] - (dfull1[b] * v + c))

    e0 = 0
    for _ in range(NU - 1):
        sweep0(e0, x0)
        e0 += 1
        pack(x0, send0, sends0, e0)
        start(level0, e0)
        own_ext(x0, ext0, nb)

    for g in range(1, g1):
        bulk_start(g)
    drain(2)
    l_cinv.wait()

    @pl.when(solving)
    def _():
        cin[my_slot] = cinv[...]
        recva[me] = aggf[...]

    l_pro0.wait()
    for b in range(nb):
        h, t = two_terms(pro0[b])
        down0[b * bs : (b + 1) * bs, :bs] = h
        down0[b * bs : (b + 1) * bs, bs:] = t
    l_blocks1.wait()
    for b in range(nb1):
        split_blocks(b, blocks1, wide1, k1)
    l_diag1.wait()
    for b in range(nb1):
        d = jnp.broadcast_to(diag1[b : b + 1, :], (loads, bs))
        dfull1[b] = d
        wfull1[b] = OMEGA / d

    finish(level0, e0)
    hear_far(0)
    tell_far(1)
    with jax.named_scope("resid0"):
        ghost_ext(recv0, ext0, nb, e0)
        for b in range(nb):
            c = coupled(b, cols0, ext0, wide0, k0)
            r = rhs[b] - (dfull0[b] * x0[b] + c)
            parts = [jnp.where(agg0[b] == a, r, 0.0) for a in range(nb1)]
            res0[:, b * bs : (b + 1) * bs] = stacked(jnp.concatenate(parts, axis=0))
        q = folded(res0[...], down0[...])
    e0 += 1

    for b in range(nb1):
        low = b * loads
        high = (nb1 + b) * loads
        total = q[low : low + loads] + q[high : high + loads]
        b1[b] = total
        x1[b] = wfull1[b] * total
    pack(x1, send1, sends1, 0, True)
    start(level1, 0)
    own_ext(x1, ext1, nb1)
    seat_start(0)
    drain(2)
    for b in range(nb1):
        h, t = two_terms(pro1[b])
        down1[b, :, :bs] = h
        down1[b, :, bs:] = t
        h, t = two_terms(pro1[b].T)
        up1[b, :, :bs] = h
        up1[b, :, bs:] = t
    for b in range(nb1):
        twice = jnp.concatenate([down1[b], down1[b]], axis=0)

        def fold(i, carry):
            at = pl.ds(pl.multiple_of(i * bs, bs), bs)
            h, t = two_terms(folded(wide1[b, at], twice))
            folded1[b, at, :bs] = h
            folded1[b, at, bs:] = t
            return carry

        lax.fori_loop(0, k1, fold, 0, unroll=7)
    for b in range(nb):
        h, t = two_terms(pro0[b].T)
        up0[b, :, :bs] = h
        up0[b, :, bs:] = t
    e1 = 0
    for _ in range(NU - 1):
        finish(level1, e1)
        if e1 == 0:
            hear_far(1)
        ghost_ext(recv1, ext1, nb1, e1)
        sweep1(b1, x1)
        e1 += 1
        pack(x1, send1, sends1, e1, True)
        start(level1, e1)
        drain(2)
        own_ext(x1, ext1, nb1)

    for share in range(1, shares):
        seat_start(share)

    @pl.when(solving)
    def _():
        seat_ready(0)

    base = [
        joined(stacked(b1[b] - dfull1[b] * x1[b]), down1[b], loads) for b in range(nb1)
    ]
    finish(level1, e1)
    to_solvers(aggf, recva, s_asend, 0)
    with jax.named_scope("resid1"):
        ghost_ext(recv1, ext1, nb1, e1)
        for b in range(nb1):
            c = coupled(b, cols1, ext1, folded1, k1)
            mine[b * loads : (b + 1) * loads, :] = base[b] - c

    to_solvers(mine, recvc, s_msend, 1)

    @pl.when(solving)
    def _():
        recvc[me] = mine[...]

    @pl.when(solving)
    def _():
        for share in range(1, shares):
            seat_ready(share)
        with jax.named_scope("waitC1"):
            all_bytes(recva, n - 1, s_brecv.at[0])
            all_bytes(recvc, n - 1, s_brecv.at[1])
        index = lax.broadcasted_iota(jnp.int32, (ncb, nb1 * loads, bs), 0).astype(F32)

        def collect(d, total):
            name = recva[d]
            name = jnp.concatenate(
                [jnp.broadcast_to(name[b : b + 1], (loads, bs)) for b in range(nb1)], axis=0
            )
            return total + jnp.where(name[None] == index, recvc[d][None], 0.0)

        total = lax.fori_loop(
            0, n, collect, jnp.zeros((ncb, nb1 * loads, bs), F32), unroll=8
        )
        lhs = jnp.concatenate([stacked(total[c]) for c in range(ncb)], axis=1)
        own = folded(lhs, wide2[...])
        rows = [own[i * loads : (i + 1) * loads] for i in range(2 * nb1)]
        own = functools.reduce(lambda a, b: a + b, rows)
        for m in range(pair):
            xs[m] = own[:, m * bs : (m + 1) * bs]

        def tell(r, c):
            pltpu.make_async_remote_copy(
                src_ref=xs, dst_ref=recvx.at[my_place],
                send_sem=s_xsend.at[0], recv_sem=s_brecv.at[2],
                device_id=(r, c), device_id_type=MESH,
            ).start()

        half = n_col // 2
        for i in range(1, n_col):
            step = half + (i // 2 if i % 2 else -(i // 2))
            c = wrapped(col + step, n_col)
            for j in range(n_row):
                tell(wrapped(row + (j + 1) % n_row, n_row), c)
        for j in range(1, n_row):
            tell(wrapped(row + j, n_row), col)
        recvx[my_place] = xs[...]

    for d, (_, _, comes) in enumerate(directions):
        for g in range(g1):
            @pl.when(comes)
            def _():
                bulk_copy(d, g, (row, col)).wait_recv()

            h, t = two_terms(precv[d, g, :bs].T)
            up1[nb1 + d * g1 + g, :, :bs] = h
            up1[nb1 + d * g1 + g, :, bs:] = t

    @pl.when(solving)
    def _():
        with jax.named_scope("waitC2"):
            if ns > 1:
                all_bytes(recvx, ns - 1, s_brecv.at[2])

    @pl.when(jnp.logical_not(solving))
    def _():
        with jax.named_scope("waitC2"):
            all_bytes(recvx, ns, s_brecv.at[2])

    names = [jnp.broadcast_to(aggf[b : b + 1], (loads, bs)) for b in range(nb1)]
    names += [precv[d, g, bs : bs + loads] for d in range(4) for g in range(g1)]
    names = jnp.stack(names)

    def pick(tier, pieces):
        for m in range(pair):
            for group in range(groups):
                at = ((tier * pair + m) * groups + group).astype(F32)
                block = recvx[tier * groups + group, m]
                pieces = pieces + jnp.where(names == at, block[None], 0.0)
        return pieces

    pieces = lax.fori_loop(0, n_row // pair, pick, jnp.zeros(names.shape, F32), unroll=2)
    for b in range(nb1):
        x1[b] = x1[b] + joined(stacked(pieces[b]), up1[b], loads)
    for d in range(4):
        for g in range(g1):
            v = nb1 + d * g1 + g
            ghost = recv1[e1, d, g] + joined(stacked(pieces[v]), up1[v], loads)
            ext1[v] = stacked(ghost)
    e1 += 1

    for i in range(NU):
        own_ext(x1, ext1, nb1)
        if i > 0:
            finish(level1, e1)
            ghost_ext(recv1, ext1, nb1, e1)
            e1 += 1
        sweep1(b1, x1)
        if i < NU - 1:
            pack(x1, send1, sends1, e1, True)
            start(level1, e1)
            drain(2)

    own_ext(x1, ext1, nb1)
    for b in range(nb):
        x0[b] = x0[b] + joined(ext1[agg0[b]], up0[b], loads)
    for i in range(NU):
        pack(x0, send0, sends0, e0)
        start(level0, e0)
        own_ext(x0, ext0, nb)
        drain(2)
        if i == NU - 1:
            for d, (goes, there, _) in enumerate(directions):
                for g in range(g1):
                    @pl.when(goes)
                    def _():
                        bulk_copy(d, g, there).wait_send()

            @pl.when(jnp.logical_not(solving))
            def _():
                for share in range(shares):
                    seat_copy(my_slot, share).wait_send()
                all_bytes(recva, ns, s_asend.at[0])
                all_bytes(recvc, ns, s_msend.at[0])

            @pl.when(solving)
            def _():
                all_bytes(tally, n - 1, s_xsend.at[0])
                if ns > 1:
                    all_bytes(recva, ns - 1, s_asend.at[0])
                    all_bytes(recvc, ns - 1, s_msend.at[0])

        sweep0(e0, out if i == NU - 1 else x0)
        e0 += 1

    drain(1)


def on_device(
    rhs, diag0, blocks0, cols0, sends0, pro0, agg0, diag1, blocks1, cols1, sends1, pro1, agg1, cinv
):
    n_row, n_col = lax.axis_size("row"), lax.axis_size("col")
    n = n_row * n_col
    _, _, nb, loads, bs = rhs.shape
    nb1 = diag1.shape[2]
    k0, k1 = cols0.shape[3], cols1.shape[3]
    g0, g1 = sends0.shape[3], sends1.shape[3]
    owned, ncu = cinv.shape
    reps = bs // owned
    pair = 2 if n_row % 2 == 0 else 1
    ns = (n_row // pair) * (n_col // reps)
    shares = 2 if (ncu // bs) % 2 == 0 else 1
    tall = -(-2 * loads // 16) * 16
    floats = [a[0, 0] for a in (rhs, diag0, blocks0, pro0, diag1, blocks1, pro1)] + [cinv]
    ints = [a[0, 0] for a in (cols0, sends0, agg0, cols1)]
    ints += [sends1[0, 0].T, agg1[0, 0]]
    vm = pltpu.VMEM
    dma = pltpu.SemaphoreType.DMA
    scratch = [vm(a.shape, F32) for a in floats]
    scratch += [pltpu.SMEM(a.shape, jnp.int32) for a in ints]
    scratch += [dma((nb + 3 + len(ints),))]
    scratch += [vm((nb, k0 * bs, 2 * bs), BF16)] + [vm((nb1, k1 * bs, 2 * bs), BF16)] * 2
    scratch += [vm((nb * bs, 2 * bs), BF16), vm((nb, bs, 2 * bs), BF16)]
    scratch += [vm((nb1, bs, 2 * bs), BF16), vm((nb1 + 4 * g1, bs, 2 * bs), BF16)]
    scratch += [vm((pair * reps, owned, ncu), F32), vm((ncu, 2 * pair * bs), BF16)]
    scratch += [vm((nb, loads, bs), F32)] * 2
    scratch += [vm((nb1, loads, bs), F32)] * 2
    scratch += [vm((nb + 4 * g0, tall, bs), BF16), vm((nb1 + 4 * g1, tall, bs), BF16)]
    scratch += [vm((nb, loads, bs), F32), vm((nb1, loads, bs), F32), vm((nb1, loads, bs), F32)]
    scratch += [vm((-(-2 * nb1 * loads // 16) * 16, nb * bs), BF16)]
    scratch += [vm((2 * NU, 4, g0, loads, bs), F32)] * 2
    scratch += [vm((2 * NU - 1, 4, g1, loads, bs), F32)] * 2
    scratch += [vm((4, g1, bs + 8, bs), F32)] * 2
    scratch += [vm((nb1, bs), F32), vm((n, nb1, bs), F32)]
    scratch += [vm((nb1 * loads, bs), F32), vm((n, nb1 * loads, bs), F32)]
    scratch += [vm((pair, loads, bs), F32), vm((ns, pair, loads, bs), F32)]
    scratch += [vm((n - 1, pair, loads, bs), F32)]
    scratch += [dma((2, 4))] * 2 + [dma((4, g1))] * 2
    scratch += [dma((shares,))] * 2 + [dma((1,))] * 3 + [dma((3,))]
    scratch += [pltpu.SemaphoreType.REGULAR((2,))]
    result = pl.pallas_call(
        functools.partial(kernel, n_row, n_col, pair),
        out_shape=pltpu.VMEM((nb, loads, bs), F32),
        in_specs=[pl.BlockSpec(memory_space=pl.ANY)] * 14,
        out_specs=pl.BlockSpec(memory_space=pltpu.VMEM),
        scratch_shapes=scratch,
        compiler_params=pltpu.CompilerParams(
            collective_id=0, has_side_effects=True, vmem_limit_bytes=60 * 1024 * 1024
        ),
    )(*ints, *floats)
    return result[None, None]


def solution(mesh):
    return jax.shard_map(
        on_device,
        mesh=mesh,
        in_specs=(
            P("row", "col", None, None, None),
            P("row", "col", None, None),
            P("row", "col", None, None, None, None),
            P("row", "col", None, None),
            P("row", "col", None, None),
            P("row", "col", None, None, None),
            P("row", "col", None),
            P("row", "col", None, None),
            P("row", "col", None, None, None, None),
            P("row", "col", None, None),
            P("row", "col", None, None),
            P("row", "col", None, None, None),
            P("row", "col", None),
            P(("row", "col"), None),
        ),
        out_specs=P("row", "col", None, None, None),
        check_vma=False,
    )
```

```python
import functools

import jax
import jax.numpy as jnp
from jax import lax
from jax.experimental import pallas as pl
from jax.experimental.pallas import tpu as pltpu
from jax.sharding import PartitionSpec as P

NU = 2
OMEGA = 0.3
F32 = jnp.float32
BF16 = jnp.bfloat16
MESH = pl.DeviceIdType.MESH
NN = (((1,), (0,)), ((), ()))


def two_terms(value):
    head = value.astype(BF16)
    tail = (value - head.astype(F32)).astype(BF16)
    return head, tail


def stacked(value):
    head = value.astype(BF16).astype(F32)
    rows = 2 * value.shape[0]
    pad = -rows % 16
    parts = [head, value - head]
    if pad:
        parts.append(jnp.zeros((pad, value.shape[1]), F32))
    return jnp.concatenate(parts, axis=0).astype(BF16)


def folded(lhs, wide):
    both = lax.dot_general(lhs, wide, NN, preferred_element_type=F32)
    half = both.shape[1] // 2
    return both[:, :half] + both[:, half:]


def joined(lhs, wide, rows):
    both = folded(lhs, wide)
    return both[:rows] + both[rows : 2 * rows]


def seat_of(group, groups, reps):
    if 2 * group + 1 < groups:
        return group * reps + reps - 1
    if 2 * group + 1 > groups:
        return group * reps
    return group * reps + reps // 2


def reaches(n_row, n_col, pair, groups, reps):
    grid = [(r, c) for r in range(n_row) for c in range(n_col)]

    def beside(p, row_steps, col_steps):
        steps = [(d, 0) for d in row_steps] + [(0, d) for d in col_steps]
        spots = [(p[0] + a, p[1] + b) for a, b in steps]
        return [q for q in spots if 0 <= q[0] < n_row and 0 <= q[1] < n_col]

    def heard(known, jump):
        told = {}
        for p in grid:
            near = beside(p, (-1, 1), (-1, 1)) + (beside(p, (), (-2, 2)) if jump else [])
            told[p] = known[p].union(*[known[q] for q in near])
        return told

    first = heard({p: {p} for p in grid}, False)
    second = heard(first, False)
    early = {}
    for r, c in grid:
        far = [(r, c + d) for d in (-2, 2) if 0 <= c + d < n_col]
        early[(r, c)] = second[(r, c)].union(*[second[q] for q in far])
    third = heard(second, True)
    last = heard(heard(third, True), False)
    seats = [seat_of(group, groups, reps) for group in range(groups)]
    for r, c in grid:
        solvers = {(t, s) for t in range(pair - 1, n_row, pair) for s in seats}
        own = (r // pair * pair + pair - 1, seats[c // reps])
        if own not in early[(r, c)] or not solvers <= last[(r, c)]:
            return False
    return True


def kernel(
    n_row, n_col, pair,
    cols0_h, sends0_h, agg0_h, cols1_h, sends1_h, agg1_h,
    rhs_h, diag0_h, blocks0_h, pro0_h, diag1_h, blocks1_h, pro1_h, cinv_h,
    out,
    rhs, diag0, blocks0, pro0, diag1, blocks1, pro1, cinv,
    cols0, sends0, agg0, cols1, sends1, agg1,
    in_sem,
    wide0, wide1, folded1, down0, up0, down1, up1, cin, wide2,
    dfull0, wfull0, dfull1, wfull1,
    ext0, ext1, x0, x1, b1, res0,
    send0, recv0, send1, recv1, psend, precv,
    aggf, recva, mine, recvc, xs, recvx, tally,
    s_send, s_recv, s_psend, s_precv,
    s_cin, s_csend, s_asend, s_msend, s_xsend, s_brecv, s_far,
):
    nb, loads, bs = rhs.shape
    nb1 = diag1.shape[0]
    k0 = blocks0.shape[1]
    k1 = blocks1.shape[1]
    g1 = send1.shape[2]
    n = n_row * n_col
    owned, ncu = cinv.shape
    ncb = ncu // bs
    reps = bs // owned
    groups = n_col // reps
    ns = (n_row // pair) * groups
    row = lax.axis_index("row")
    col = lax.axis_index("col")
    me = row * n_col + col

    seats = [seat_of(group, groups, reps) for group in range(groups)]
    solvers = [
        (tier * pair + pair - 1, seats[group])
        for tier in range(n_row // pair) for group in range(groups)
    ]
    my_tier, my_group = row // pair, col // reps
    my_seat = jnp.int32(0)
    for group in range(groups):
        my_seat = jnp.where(my_group == group, seats[group], my_seat)
    solving = (lax.rem(row, pair) == pair - 1) & (col == my_seat)
    my_place = my_tier * groups + my_group
    my_slot = lax.rem(row, pair) * reps + lax.rem(col, reps)

    directions = (
        (row < n_row - 1, (row + 1, col), row > 0),
        (row > 0, (row - 1, col), row < n_row - 1),
        (col < n_col - 1, (row, col + 1), col > 0),
        (col > 0, (row, col - 1), col < n_col - 1),
    )

    def wrapped(i, size):
        return jnp.where(i >= size, i - size, i)

    barrier = pltpu.get_barrier_semaphore()
    relayed = reaches(n_row, n_col, pair, groups, reps)

    def greet(r, c):
        pl.semaphore_signal(barrier, inc=1, device_id=(r, c), device_id_type=MESH)

    loading = []

    def load(source, target):
        copy = pltpu.make_async_copy(source, target, in_sem.at[len(loading) % in_sem.shape[0]])
        loading.append(copy)
        copy.start()
        return copy

    if relayed:
        for goes, (r, c) in [(goes, there) for goes, there, _ in directions]:
            @pl.when(goes)
            def _():
                greet(r, c)
    else:
        for i in range(1, n_row):
            greet(wrapped(row + i, n_row), col)

    l_ints = [load(sends0_h, sends0), load(sends1_h, sends1), load(agg1_h, agg1)]
    l_rhs = load(rhs_h, rhs)
    l_diag0 = load(diag0_h, diag0)
    l_pro1 = load(pro1_h, pro1)
    step = 2 if nb % 2 == 0 else 1
    l_blocks0 = [
        load(blocks0_h.at[pl.ds(b, step)], blocks0.at[pl.ds(b, step)]) for b in range(0, nb, step)
    ]

    if not relayed:
        def greet_line(i, carry):
            c = wrapped(col + i, n_col)
            for r in range(n_row):
                greet(r, c)
            return carry

        lax.fori_loop(1, n_col, greet_line, 0, unroll=min(n_col - 1, 7))

    for d, (_, _, comes) in enumerate(directions):
        @pl.when(jnp.logical_not(comes))
        def _():
            for e in range(recv0.shape[0]):
                recv0[e, d] = jnp.zeros(recv0.shape[2:], F32)
            for e in range(recv1.shape[0]):
                recv1[e, d] = jnp.zeros(recv1.shape[2:], F32)
            precv[d] = jnp.zeros(precv.shape[1:], F32)

    order = []

    def halo_copy(level, e, d, there):
        send, recv = level
        turn = order.index((level is level1, e)) % 2
        return pltpu.make_async_remote_copy(
            src_ref=send.at[e, d], dst_ref=recv.at[e, d],
            send_sem=s_send.at[turn, d], recv_sem=s_recv.at[turn, d],
            device_id=there, device_id_type=MESH,
        )

    def pack(x, send, sends, e, flip=False):
        for d in range(4):
            for g in range(send.shape[2]):
                send[e, d, g] = x[sends[g, d] if flip else sends[d, g]]

    def start(level, e):
        order.append((level is level1, e))
        for d in (2, 3, 0, 1):
            goes, there, _ = directions[d]

            @pl.when(goes)
            def _():
                halo_copy(level, e, d, there).start()

    def finish(level, e):
        with jax.named_scope("finish"):
            for d, (_, there, comes) in enumerate(directions):
                @pl.when(comes)
                def _():
                    halo_copy(level, e, d, (row, col)).wait_recv()

    def drain(back):
        if back > len(order):
            return
        upper, e = order[-back]
        for d, (goes, there, _) in enumerate(directions):
            @pl.when(goes)
            def _():
                halo_copy(level1 if upper else level0, e, d, there).wait_send()

    level0 = (send0, recv0)
    level1 = (send1, recv1)

    def bulk_copy(d, g, there):
        return pltpu.make_async_remote_copy(
            src_ref=psend.at[d, g], dst_ref=precv.at[d, g],
            send_sem=s_psend.at[d], recv_sem=s_precv.at[d],
            device_id=there, device_id_type=MESH,
        )

    def bulk_start(g):
        for d, (goes, there, _) in enumerate(directions):
            psend[d, g, :bs] = pro1[sends1[g, d]]
            psend[d, g, bs:] = jnp.full((8, bs), agg1[sends1[g, d]].astype(F32))

            @pl.when(goes)
            def _():
                bulk_copy(d, g, there).start()

    def own_ext(x, ext, count):
        for b in range(count):
            ext[b] = stacked(x[b])

    def ghost_ext(recv, ext, count, e):
        ghosts = recv.shape[2]
        for d in range(4):
            for g in range(ghosts):
                ext[count + d * ghosts + g] = stacked(recv[e, d, g])

    def coupled(b, cols, ext, wide, k):
        lhs = jnp.concatenate([ext[cols[b, i]] for i in range(k)], axis=1)
        return joined(lhs, wide[b], loads)

    def split_blocks(b, blocks, wide, k):
        def one(i, carry):
            h, t = two_terms(blocks[b, i].T)
            at = pl.ds(pl.multiple_of(i * bs, bs), bs)
            wide[b, at, :bs] = h
            wide[b, at, bs:] = t
            return carry

        lax.fori_loop(0, k, one, 0, unroll=7)

    def arrive(b):
        if b % step == 0:
            l_blocks0[b // step].wait()
        split_blocks(b, blocks0, wide0, k0)

    shares = s_csend.shape[0]
    width = ncu // shares

    def seat_copy(slot, share):
        lanes = pl.ds(share * width, width)
        return pltpu.make_async_remote_copy(
            src_ref=cinv.at[:, lanes], dst_ref=cin.at[slot, :, lanes],
            send_sem=s_csend.at[share], recv_sem=s_cin.at[share],
            device_id=(my_tier * pair + pair - 1, my_seat), device_id_type=MESH,
        )

    def seat_start(share):
        @pl.when(jnp.logical_not(solving))
        def _():
            seat_copy(my_slot, share).start()

    def seat_ready(share):
        if pair * reps > 1:
            part = cin.at[pl.ds(0, pair * reps - 1), :, pl.ds(share * width, width)]
            pltpu.make_async_copy(part, part, s_cin.at[share]).wait()

        def one(c, carry):
            at = pl.ds(pl.multiple_of(c * bs, bs), bs)
            for m in range(pair):
                piece = cin[m * reps : (m + 1) * reps, :, at].reshape(bs, bs)
                h, t = two_terms(piece.T)
                wide2[at, m * bs : (m + 1) * bs] = h
                wide2[at, (pair + m) * bs : (pair + m + 1) * bs] = t
            return carry

        first = share * (ncb // shares)
        lax.fori_loop(first, first + ncb // shares, one, 0, unroll=4 if ncb // shares % 4 == 0 else 1)

    l_rhs.wait()
    l_diag0.wait()
    for b in range(nb):
        d = jnp.broadcast_to(diag0[b : b + 1, :], (loads, bs))
        w = OMEGA / d
        dfull0[b] = d
        wfull0[b] = w
        x0[b] = w * rhs[b]
    for copy in l_ints:
        copy.wait()
    pack(x0, send0, sends0, 0)
    with jax.named_scope("barrier"):
        if relayed:
            count = jnp.int32(0)
            for _, _, comes in directions:
                count = count + jnp.where(comes, 1, 0)
            pl.semaphore_wait(barrier, count)
        else:
            pl.semaphore_wait(barrier, n - 1)
    start(level0, 0)
    l_pro1.wait()
    bulk_start(0)
    l_late = [
        load(source, target)
        for source, target in (
            (cols0_h, cols0), (agg0_h, agg0), (cols1_h, cols1), (cinv_h, cinv), (pro0_h, pro0),
            (diag1_h, diag1),
        )
    ]
    own_ext(x0, ext0, nb)
    for b in range(nb1):
        aggf[b : b + 1, :] = jnp.full((1, bs), agg1[b].astype(F32))
    arrive(0)
    l_blocks1 = load(blocks1_h, blocks1)
    mixed = 3
    for b in range(1, nb - mixed):
        arrive(b)
    for copy in l_late[:3]:
        copy.wait()
    if mixed:
        for b in range(nb - mixed, nb):
            if b % step == 0:
                l_blocks0[b // step].wait()

    def tell_far(jump):
        if relayed:
            for goes, c in ((col + 2 < n_col, col + 2), (col > 1, col - 2)):
                @pl.when(goes)
                def _():
                    pl.semaphore_signal(
                        s_far.at[jump], inc=1, device_id=(row, c), device_id_type=MESH
                    )

    def hear_far(jump):
        if relayed:
            count = jnp.where(col + 2 < n_col, 1, 0) + jnp.where(col > 1, 1, 0)
            pl.semaphore_wait(s_far.at[jump], count)

    def to_solvers(src, dst, s_out, which):
        for r, c in solvers:
            @pl.when((row != r) | (col != c))
            def _():
                pltpu.make_async_remote_copy(
                    src_ref=src, dst_ref=dst.at[me],
                    send_sem=s_out.at[0], recv_sem=s_brecv.at[which],
                    device_id=(r, c), device_id_type=MESH,
                ).start()

    def all_bytes(dst, count, sem):
        part = dst.at[pl.ds(0, count)]
        pltpu.make_async_copy(part, part, sem).wait()

    def sweep0(e, into):
        finish(level0, e)
        if e == 0:
            tell_far(0)
        with jax.named_scope("sweep0"):
            ghost_ext(recv0, ext0, nb, e)
            rest = []
            if e == 0:
                rest = [(b, i) for b in range(nb - mixed, nb) for i in range(k0)]
            each = -(-len(rest) // max(nb - mixed, 1))
            for b in range(nb):
                for late, i in rest[b * each : (b + 1) * each]:
                    h, t = two_terms(blocks0[late, i].T)
                    wide0[late, i * bs : (i + 1) * bs, :bs] = h
                    wide0[late, i * bs : (i + 1) * bs, bs:] = t
                c = coupled(b, cols0, ext0, wide0, k0)
                v = x0[b]
                into[b] = v + wfull0[b] * (rhs[b] - (dfull0[b] * v + c))

    def sweep1(right, into):
        with jax.named_scope("sweep1"):
            for b in range(nb1):
                c = coupled(b, cols1, ext1, wide1, k1)
                v = x1[b]
                into[b] = v + wfull1[b] * (right[b] - (dfull1[b] * v + c))

    e0 = 0
    for _ in range(NU - 1):
        sweep0(e0, x0)
        e0 += 1
        pack(x0, send0, sends0, e0)
        start(level0, e0)
        own_ext(x0, ext0, nb)

    drain(2)

    l_late[4].wait()
    for b in range(nb):
        h, t = two_terms(pro0[b])
        down0[b * bs : (b + 1) * bs, :bs] = h
        down0[b * bs : (b + 1) * bs, bs:] = t
    l_blocks1.wait()
    for b in range(nb1):
        split_blocks(b, blocks1, wide1, k1)
    l_late[5].wait()
    for b in range(nb1):
        d = jnp.broadcast_to(diag1[b : b + 1, :], (loads, bs))
        dfull1[b] = d
        wfull1[b] = OMEGA / d

    hear_far(0)
    l_late[3].wait()

    @pl.when(solving)
    def _():
        cin[my_slot] = cinv[...]
        recva[me] = aggf[...]

    seat_start(0)
    finish(level0, e0)
    tell_far(1)
    with jax.named_scope("resid0"):
        ghost_ext(recv0, ext0, nb, e0)
        for b in range(nb):
            c = coupled(b, cols0, ext0, wide0, k0)
            r = rhs[b] - (dfull0[b] * x0[b] + c)
            parts = [jnp.where(agg0[b] == a, r, 0.0) for a in range(nb1)]
            res0[:, b * bs : (b + 1) * bs] = stacked(jnp.concatenate(parts, axis=0))
        q = folded(res0[...], down0[...])
    e0 += 1

    for b in range(nb1):
        low = b * loads
        high = (nb1 + b) * loads
        total = q[low : low + loads] + q[high : high + loads]
        b1[b] = total
        x1[b] = wfull1[b] * total
    pack(x1, send1, sends1, 0, True)
    start(level1, 0)
    own_ext(x1, ext1, nb1)
    for share in range(1, shares):
        seat_start(share)
    drain(2)
    for b in range(nb1):
        h, t = two_terms(pro1[b])
        down1[b, :, :bs] = h
        down1[b, :, bs:] = t
        h, t = two_terms(pro1[b].T)
        up1[b, :, :bs] = h
        up1[b, :, bs:] = t
    for b in range(nb1):
        twice = jnp.concatenate([down1[b], down1[b]], axis=0)

        def fold(i, carry):
            at = pl.ds(pl.multiple_of(i * bs, bs), bs)
            h, t = two_terms(folded(wide1[b, at], twice))
            folded1[b, at, :bs] = h
            folded1[b, at, bs:] = t
            return carry

        lax.fori_loop(0, k1, fold, 0, unroll=7)
    for b in range(nb):
        h, t = two_terms(pro0[b].T)
        up0[b, :, :bs] = h
        up0[b, :, bs:] = t
    e1 = 0
    for _ in range(NU - 1):
        finish(level1, e1)
        if e1 == 0:
            hear_far(1)
        ghost_ext(recv1, ext1, nb1, e1)
        sweep1(b1, x1)
        e1 += 1
        pack(x1, send1, sends1, e1, True)
        start(level1, e1)
        drain(2)
        own_ext(x1, ext1, nb1)

    @pl.when(solving)
    def _():
        for share in range(shares):
            seat_ready(share)

    base = [
        joined(stacked(b1[b] - dfull1[b] * x1[b]), down1[b], loads) for b in range(nb1)
    ]
    finish(level1, e1)
    to_solvers(aggf, recva, s_asend, 0)
    with jax.named_scope("resid1"):
        ghost_ext(recv1, ext1, nb1, e1)
        for b in range(nb1):
            c = coupled(b, cols1, ext1, folded1, k1)
            mine[b * loads : (b + 1) * loads, :] = base[b] - c

    to_solvers(mine, recvc, s_msend, 1)
    for g in range(1, g1):
        for d, (goes, there, _) in enumerate(directions):
            @pl.when(goes)
            def _():
                bulk_copy(d, g - 1, there).wait_send()
        bulk_start(g)

    @pl.when(solving)
    def _():
        recvc[me] = mine[...]

    @pl.when(solving)
    def _():
        with jax.named_scope("waitC1"):
            all_bytes(recva, n - 1, s_brecv.at[0])
            all_bytes(recvc, n - 1, s_brecv.at[1])
        index = lax.broadcasted_iota(jnp.int32, (ncb, nb1 * loads, bs), 0).astype(F32)

        def collect(d, total):
            name = recva[d]
            name = jnp.concatenate(
                [jnp.broadcast_to(name[b : b + 1], (loads, bs)) for b in range(nb1)], axis=0
            )
            return total + jnp.where(name[None] == index, recvc[d][None], 0.0)

        total = lax.fori_loop(
            0, n, collect, jnp.zeros((ncb, nb1 * loads, bs), F32), unroll=8
        )
        lhs = jnp.concatenate([stacked(total[c]) for c in range(ncb)], axis=1)
        own = folded(lhs, wide2[...])
        rows = [own[i * loads : (i + 1) * loads] for i in range(2 * nb1)]
        own = functools.reduce(lambda a, b: a + b, rows)
        for m in range(pair):
            xs[m] = own[:, m * bs : (m + 1) * bs]

        def tell(r, c):
            pltpu.make_async_remote_copy(
                src_ref=xs, dst_ref=recvx.at[my_place],
                send_sem=s_xsend.at[0], recv_sem=s_brecv.at[2],
                device_id=(r, c), device_id_type=MESH,
            ).start()

        half = n_col // 2
        for i in range(1, n_col):
            step = half + (i // 2 if i % 2 else -(i // 2))
            c = wrapped(col + step, n_col)
            for j in range(n_row):
                tell(wrapped(row + (j + 1) % n_row, n_row), c)
        for j in range(1, n_row):
            tell(wrapped(row + j, n_row), col)
        recvx[my_place] = xs[...]

    for d, (_, _, comes) in enumerate(directions):
        @pl.when(comes)
        def _():
            pltpu.make_async_copy(precv.at[d], precv.at[d], s_precv.at[d]).wait()

        for g in range(g1):
            h, t = two_terms(precv[d, g, :bs].T)
            up1[nb1 + d * g1 + g, :, :bs] = h
            up1[nb1 + d * g1 + g, :, bs:] = t

    @pl.when(solving)
    def _():
        with jax.named_scope("waitC2"):
            if ns > 1:
                all_bytes(recvx, ns - 1, s_brecv.at[2])

    @pl.when(jnp.logical_not(solving))
    def _():
        with jax.named_scope("waitC2"):
            all_bytes(recvx, ns, s_brecv.at[2])

    names = [jnp.broadcast_to(aggf[b : b + 1], (loads, bs)) for b in range(nb1)]
    names += [precv[d, g, bs : bs + loads] for d in range(4) for g in range(g1)]
    names = jnp.stack(names)

    def pick(tier, pieces):
        for m in range(pair):
            for group in range(groups):
                at = ((tier * pair + m) * groups + group).astype(F32)
                block = recvx[tier * groups + group, m]
                pieces = pieces + jnp.where(names == at, block[None], 0.0)
        return pieces

    pieces = lax.fori_loop(0, n_row // pair, pick, jnp.zeros(names.shape, F32), unroll=2)
    for b in range(nb1):
        x1[b] = x1[b] + joined(stacked(pieces[b]), up1[b], loads)
    for d in range(4):
        for g in range(g1):
            v = nb1 + d * g1 + g
            ghost = recv1[e1, d, g] + joined(stacked(pieces[v]), up1[v], loads)
            ext1[v] = stacked(ghost)
    e1 += 1

    for i in range(NU):
        own_ext(x1, ext1, nb1)
        if i > 0:
            finish(level1, e1)
            ghost_ext(recv1, ext1, nb1, e1)
            e1 += 1
        sweep1(b1, x1)
        if i < NU - 1:
            pack(x1, send1, sends1, e1, True)
            start(level1, e1)
            drain(2)

    own_ext(x1, ext1, nb1)
    for b in range(nb):
        x0[b] = x0[b] + joined(ext1[agg0[b]], up0[b], loads)
    for i in range(NU):
        pack(x0, send0, sends0, e0)
        start(level0, e0)
        own_ext(x0, ext0, nb)
        drain(2)
        if i == NU - 1:
            for d, (goes, there, _) in enumerate(directions):
                @pl.when(goes)
                def _():
                    bulk_copy(d, g1 - 1, there).wait_send()

            @pl.when(jnp.logical_not(solving))
            def _():
                for share in range(shares):
                    seat_copy(my_slot, share).wait_send()
                all_bytes(recva, ns, s_asend.at[0])
                all_bytes(recvc, ns, s_msend.at[0])

            @pl.when(solving)
            def _():
                all_bytes(tally, n - 1, s_xsend.at[0])
                if ns > 1:
                    all_bytes(recva, ns - 1, s_asend.at[0])
                    all_bytes(recvc, ns - 1, s_msend.at[0])

        sweep0(e0, out if i == NU - 1 else x0)
        e0 += 1

    drain(1)


def on_device(
    rhs, diag0, blocks0, cols0, sends0, pro0, agg0, diag1, blocks1, cols1, sends1, pro1, agg1, cinv
):
    n_row, n_col = lax.axis_size("row"), lax.axis_size("col")
    n = n_row * n_col
    _, _, nb, loads, bs = rhs.shape
    nb1 = diag1.shape[2]
    k0, k1 = cols0.shape[3], cols1.shape[3]
    g0, g1 = sends0.shape[3], sends1.shape[3]
    owned, ncu = cinv.shape
    reps = bs // owned
    pair = 2 if n_row % 2 == 0 else 1
    ns = (n_row // pair) * (n_col // reps)
    shares = 2 if (ncu // bs) % 2 == 0 else 1
    tall = -(-2 * loads // 16) * 16
    floats = [a[0, 0] for a in (rhs, diag0, blocks0, pro0, diag1, blocks1, pro1)] + [cinv]
    ints = [a[0, 0] for a in (cols0, sends0, agg0, cols1)]
    ints += [sends1[0, 0].T, agg1[0, 0]]
    vm = pltpu.VMEM
    dma = pltpu.SemaphoreType.DMA
    scratch = [vm(a.shape, F32) for a in floats]
    scratch += [pltpu.SMEM(a.shape, jnp.int32) for a in ints]
    scratch += [dma((6 + (nb // 2 if nb % 2 == 0 else nb),))]
    scratch += [vm((nb, k0 * bs, 2 * bs), BF16)] + [vm((nb1, k1 * bs, 2 * bs), BF16)] * 2
    scratch += [vm((nb * bs, 2 * bs), BF16), vm((nb, bs, 2 * bs), BF16)]
    scratch += [vm((nb1, bs, 2 * bs), BF16), vm((nb1 + 4 * g1, bs, 2 * bs), BF16)]
    scratch += [vm((pair * reps, owned, ncu), F32), vm((ncu, 2 * pair * bs), BF16)]
    scratch += [vm((nb, loads, bs), F32)] * 2
    scratch += [vm((nb1, loads, bs), F32)] * 2
    scratch += [vm((nb + 4 * g0, tall, bs), BF16), vm((nb1 + 4 * g1, tall, bs), BF16)]
    scratch += [vm((nb, loads, bs), F32), vm((nb1, loads, bs), F32), vm((nb1, loads, bs), F32)]
    scratch += [vm((-(-2 * nb1 * loads // 16) * 16, nb * bs), BF16)]
    scratch += [vm((2 * NU, 4, g0, loads, bs), F32)] * 2
    scratch += [vm((2 * NU - 1, 4, g1, loads, bs), F32)] * 2
    scratch += [vm((4, g1, bs + 8, bs), F32)] * 2
    scratch += [vm((nb1, bs), F32), vm((n, nb1, bs), F32)]
    scratch += [vm((nb1 * loads, bs), F32), vm((n, nb1 * loads, bs), F32)]
    scratch += [vm((pair, loads, bs), F32), vm((ns, pair, loads, bs), F32)]
    scratch += [vm((n - 1, pair, loads, bs), F32)]
    scratch += [dma((2, 4))] * 2 + [dma((4,))] * 2
    scratch += [dma((shares,))] * 2 + [dma((1,))] * 3 + [dma((3,))]
    scratch += [pltpu.SemaphoreType.REGULAR((2,))]
    result = pl.pallas_call(
        functools.partial(kernel, n_row, n_col, pair),
        out_shape=pltpu.VMEM((nb, loads, bs), F32),
        in_specs=[pl.BlockSpec(memory_space=pl.ANY)] * 14,
        out_specs=pl.BlockSpec(memory_space=pltpu.VMEM),
        scratch_shapes=scratch,
        compiler_params=pltpu.CompilerParams(
            collective_id=0, has_side_effects=True, vmem_limit_bytes=60 * 1024 * 1024
        ),
    )(*ints, *floats)
    return result[None, None]


def solution(mesh):
    return jax.shard_map(
        on_device,
        mesh=mesh,
        in_specs=(
            P("row", "col", None, None, None),
            P("row", "col", None, None),
            P("row", "col", None, None, None, None),
            P("row", "col", None, None),
            P("row", "col", None, None),
            P("row", "col", None, None, None),
            P("row", "col", None),
            P("row", "col", None, None),
            P("row", "col", None, None, None, None),
            P("row", "col", None, None),
            P("row", "col", None, None),
            P("row", "col", None, None, None),
            P("row", "col", None),
            P(("row", "col"), None),
        ),
        out_specs=P("row", "col", None, None, None),
        check_vma=False,
    )
```

```python
import functools

import jax
import jax.numpy as jnp
from jax import lax
from jax.experimental import pallas as pl
from jax.experimental.pallas import tpu as pltpu
from jax.sharding import PartitionSpec as P

NU = 2
OMEGA = 0.3
F32 = jnp.float32
BF16 = jnp.bfloat16
MESH = pl.DeviceIdType.MESH
NN = (((1,), (0,)), ((), ()))


def two_terms(value):
    head = value.astype(BF16)
    tail = (value - head.astype(F32)).astype(BF16)
    return head, tail


def stacked(value):
    head = value.astype(BF16).astype(F32)
    rows = 2 * value.shape[0]
    pad = -rows % 16
    parts = [head, value - head]
    if pad:
        parts.append(jnp.zeros((pad, value.shape[1]), F32))
    return jnp.concatenate(parts, axis=0).astype(BF16)


def folded(lhs, wide):
    both = lax.dot_general(lhs, wide, NN, preferred_element_type=F32)
    half = both.shape[1] // 2
    return both[:, :half] + both[:, half:]


def joined(lhs, wide, rows):
    both = folded(lhs, wide)
    return both[:rows] + both[rows : 2 * rows]


def seat_of(group, groups, reps):
    if 2 * group + 1 < groups:
        return group * reps + reps - 1
    if 2 * group + 1 > groups:
        return group * reps
    return group * reps + reps // 2


def reaches(n_row, n_col, pair, groups, reps):
    grid = [(r, c) for r in range(n_row) for c in range(n_col)]

    def beside(p, row_steps, col_steps):
        steps = [(d, 0) for d in row_steps] + [(0, d) for d in col_steps]
        spots = [(p[0] + a, p[1] + b) for a, b in steps]
        return [q for q in spots if 0 <= q[0] < n_row and 0 <= q[1] < n_col]

    def heard(known, jump):
        told = {}
        for p in grid:
            near = beside(p, (-1, 1), (-1, 1)) + (beside(p, (), (-2, 2)) if jump else [])
            told[p] = known[p].union(*[known[q] for q in near])
        return told

    first = heard({p: {p} for p in grid}, False)
    second = heard(first, False)
    early = {}
    for r, c in grid:
        far = [(r, c + d) for d in (-2, 2) if 0 <= c + d < n_col]
        early[(r, c)] = second[(r, c)].union(*[second[q] for q in far])
    third = heard(second, True)
    last = heard(heard(third, True), False)
    seats = [seat_of(group, groups, reps) for group in range(groups)]
    for r, c in grid:
        solvers = {(t, s) for t in range(pair - 1, n_row, pair) for s in seats}
        own = (r // pair * pair + pair - 1, seats[c // reps])
        if own not in early[(r, c)] or not solvers <= last[(r, c)]:
            return False
    return True


def kernel(
    n_row, n_col, pair,
    cols0_h, sends0_h, agg0_h, cols1_h, sends1_h, agg1_h,
    rhs_h, diag0_h, blocks0_h, pro0_h, diag1_h, blocks1_h, pro1_h, cinv_h,
    out,
    rhs, diag0, blocks0, pro0, diag1, blocks1, pro1, cinv,
    cols0, sends0, agg0, cols1, sends1, agg1,
    in_sem,
    wide0, wide1, folded1, lifted1, down0, up0, down1, up1, cin, wide2,
    dfull0, wfull0, dfull1, wfull1,
    ext0, ext1, pext, x0, x1, b1, past1, res0,
    send0, recv0, send1, recv1, psend, precv,
    aggf, recva, mine, recvc, xs, recvx, tally,
    s_send, s_recv, s_psend, s_precv,
    s_cin, s_csend, s_asend, s_msend, s_xsend, s_brecv, s_far,
):
    nb, loads, bs = rhs.shape
    nb1 = diag1.shape[0]
    k0 = blocks0.shape[1]
    k1 = blocks1.shape[1]
    g1 = send1.shape[2]
    n = n_row * n_col
    owned, ncu = cinv.shape
    ncb = ncu // bs
    reps = bs // owned
    groups = n_col // reps
    ns = (n_row // pair) * groups
    row = lax.axis_index("row")
    col = lax.axis_index("col")
    me = row * n_col + col

    seats = [seat_of(group, groups, reps) for group in range(groups)]
    solvers = [
        (tier * pair + pair - 1, seats[group])
        for tier in range(n_row // pair) for group in range(groups)
    ]
    my_tier, my_group = row // pair, col // reps
    my_seat = jnp.int32(0)
    for group in range(groups):
        my_seat = jnp.where(my_group == group, seats[group], my_seat)
    solving = (lax.rem(row, pair) == pair - 1) & (col == my_seat)
    my_place = my_tier * groups + my_group
    my_slot = lax.rem(row, pair) * reps + lax.rem(col, reps)

    directions = (
        (row < n_row - 1, (row + 1, col), row > 0),
        (row > 0, (row - 1, col), row < n_row - 1),
        (col < n_col - 1, (row, col + 1), col > 0),
        (col > 0, (row, col - 1), col < n_col - 1),
    )

    def wrapped(i, size):
        return jnp.where(i >= size, i - size, i)

    barrier = pltpu.get_barrier_semaphore()
    relayed = reaches(n_row, n_col, pair, groups, reps)

    def greet(r, c):
        pl.semaphore_signal(barrier, inc=1, device_id=(r, c), device_id_type=MESH)

    loading = []

    def load(source, target):
        copy = pltpu.make_async_copy(source, target, in_sem.at[len(loading) % in_sem.shape[0]])
        loading.append(copy)
        copy.start()
        return copy

    if relayed:
        for goes, (r, c) in [(goes, there) for goes, there, _ in directions]:
            @pl.when(goes)
            def _():
                greet(r, c)
    else:
        for i in range(1, n_row):
            greet(wrapped(row + i, n_row), col)

    l_ints = [load(sends0_h, sends0), load(sends1_h, sends1), load(agg1_h, agg1)]
    l_rhs = load(rhs_h, rhs)
    l_diag0 = load(diag0_h, diag0)
    l_pro1 = load(pro1_h, pro1)
    step = 2 if nb % 2 == 0 else 1
    l_blocks0 = [
        load(blocks0_h.at[pl.ds(b, step)], blocks0.at[pl.ds(b, step)]) for b in range(0, nb, step)
    ]

    if not relayed:
        def greet_line(i, carry):
            c = wrapped(col + i, n_col)
            for r in range(n_row):
                greet(r, c)
            return carry

        lax.fori_loop(1, n_col, greet_line, 0, unroll=min(n_col - 1, 7))

    for d, (_, _, comes) in enumerate(directions):
        @pl.when(jnp.logical_not(comes))
        def _():
            for e in range(recv0.shape[0]):
                recv0[e, d] = jnp.zeros(recv0.shape[2:], F32)
            for e in range(recv1.shape[0]):
                recv1[e, d] = jnp.zeros(recv1.shape[2:], F32)
            precv[d] = jnp.zeros(precv.shape[1:], F32)

    order = []

    def halo_copy(level, e, d, there):
        send, recv = level
        turn = order.index((level is level1, e)) % 2
        return pltpu.make_async_remote_copy(
            src_ref=send.at[e, d], dst_ref=recv.at[e, d],
            send_sem=s_send.at[turn, d], recv_sem=s_recv.at[turn, d],
            device_id=there, device_id_type=MESH,
        )

    def pack(x, send, sends, e, flip=False):
        for d in range(4):
            for g in range(send.shape[2]):
                send[e, d, g] = x[sends[g, d] if flip else sends[d, g]]

    def start(level, e):
        order.append((level is level1, e))
        for d in (2, 3, 0, 1):
            goes, there, _ = directions[d]

            @pl.when(goes)
            def _():
                halo_copy(level, e, d, there).start()

    def finish(level, e):
        with jax.named_scope("finish"):
            for d, (_, there, comes) in enumerate(directions):
                @pl.when(comes)
                def _():
                    halo_copy(level, e, d, (row, col)).wait_recv()

    def drain(back):
        if back > len(order):
            return
        upper, e = order[-back]
        for d, (goes, there, _) in enumerate(directions):
            @pl.when(goes)
            def _():
                halo_copy(level1 if upper else level0, e, d, there).wait_send()

    level0 = (send0, recv0)
    level1 = (send1, recv1)

    def bulk_copy(d, g, there):
        return pltpu.make_async_remote_copy(
            src_ref=psend.at[d, g], dst_ref=precv.at[d, g],
            send_sem=s_psend.at[d], recv_sem=s_precv.at[d],
            device_id=there, device_id_type=MESH,
        )

    def bulk_start(g):
        for d, (goes, there, _) in enumerate(directions):
            psend[d, g, :bs] = pro1[sends1[g, d]]
            psend[d, g, bs:] = jnp.full((8, bs), agg1[sends1[g, d]].astype(F32))

            @pl.when(goes)
            def _():
                bulk_copy(d, g, there).start()

    def own_ext(x, ext, count):
        for b in range(count):
            ext[b] = stacked(x[b])

    def ghost_ext(recv, ext, count, e):
        ghosts = recv.shape[2]
        for d in range(4):
            for g in range(ghosts):
                ext[count + d * ghosts + g] = stacked(recv[e, d, g])

    def coupled(b, cols, ext, wide, k):
        lhs = jnp.concatenate([ext[cols[b, i]] for i in range(k)], axis=1)
        return joined(lhs, wide[b], loads)

    def split_blocks(b, blocks, wide, k):
        def one(i, carry):
            h, t = two_terms(blocks[b, i].T)
            at = pl.ds(pl.multiple_of(i * bs, bs), bs)
            wide[b, at, :bs] = h
            wide[b, at, bs:] = t
            return carry

        lax.fori_loop(0, k, one, 0, unroll=7)

    def arrive(b):
        if b % step == 0:
            l_blocks0[b // step].wait()
        split_blocks(b, blocks0, wide0, k0)

    shares = s_csend.shape[0]
    width = ncu // shares

    def seat_copy(slot, share):
        lanes = pl.ds(share * width, width)
        return pltpu.make_async_remote_copy(
            src_ref=cinv.at[:, lanes], dst_ref=cin.at[slot, :, lanes],
            send_sem=s_csend.at[share], recv_sem=s_cin.at[share],
            device_id=(my_tier * pair + pair - 1, my_seat), device_id_type=MESH,
        )

    def seat_start(share):
        @pl.when(jnp.logical_not(solving))
        def _():
            seat_copy(my_slot, share).start()

    def seat_ready(share):
        if pair * reps > 1:
            part = cin.at[pl.ds(0, pair * reps - 1), :, pl.ds(share * width, width)]
            pltpu.make_async_copy(part, part, s_cin.at[share]).wait()

        def one(c, carry):
            at = pl.ds(pl.multiple_of(c * bs, bs), bs)
            for m in range(pair):
                piece = cin[m * reps : (m + 1) * reps, :, at].reshape(bs, bs)
                h, t = two_terms(piece.T)
                wide2[at, m * bs : (m + 1) * bs] = h
                wide2[at, (pair + m) * bs : (pair + m + 1) * bs] = t
            return carry

        first = share * (ncb // shares)
        lax.fori_loop(first, first + ncb // shares, one, 0, unroll=4 if ncb // shares % 4 == 0 else 1)

    l_rhs.wait()
    l_diag0.wait()
    for b in range(nb):
        d = jnp.broadcast_to(diag0[b : b + 1, :], (loads, bs))
        w = OMEGA / d
        dfull0[b] = d
        wfull0[b] = w
        x0[b] = w * rhs[b]
    for copy in l_ints:
        copy.wait()
    pack(x0, send0, sends0, 0)
    with jax.named_scope("barrier"):
        if relayed:
            count = jnp.int32(0)
            for _, _, comes in directions:
                count = count + jnp.where(comes, 1, 0)
            pl.semaphore_wait(barrier, count)
        else:
            pl.semaphore_wait(barrier, n - 1)
    start(level0, 0)
    l_pro1.wait()
    bulk_start(0)
    l_late = [
        load(source, target)
        for source, target in (
            (cols0_h, cols0), (agg0_h, agg0), (cols1_h, cols1), (cinv_h, cinv), (pro0_h, pro0),
            (diag1_h, diag1),
        )
    ]
    own_ext(x0, ext0, nb)
    for b in range(nb1):
        aggf[b : b + 1, :] = jnp.full((1, bs), agg1[b].astype(F32))
    arrive(0)
    l_blocks1 = load(blocks1_h, blocks1)
    mixed = 3
    for b in range(1, nb - mixed):
        arrive(b)
    for copy in l_late[:3]:
        copy.wait()
    if mixed:
        for b in range(nb - mixed, nb):
            if b % step == 0:
                l_blocks0[b // step].wait()

    def tell_far(jump):
        if relayed:
            for goes, c in ((col + 2 < n_col, col + 2), (col > 1, col - 2)):
                @pl.when(goes)
                def _():
                    pl.semaphore_signal(
                        s_far.at[jump], inc=1, device_id=(row, c), device_id_type=MESH
                    )

    def hear_far(jump):
        if relayed:
            count = jnp.where(col + 2 < n_col, 1, 0) + jnp.where(col > 1, 1, 0)
            pl.semaphore_wait(s_far.at[jump], count)

    def to_solvers(src, dst, s_out, which):
        for r, c in solvers:
            @pl.when((row != r) | (col != c))
            def _():
                pltpu.make_async_remote_copy(
                    src_ref=src, dst_ref=dst.at[me],
                    send_sem=s_out.at[0], recv_sem=s_brecv.at[which],
                    device_id=(r, c), device_id_type=MESH,
                ).start()

    def all_bytes(dst, count, sem):
        part = dst.at[pl.ds(0, count)]
        pltpu.make_async_copy(part, part, sem).wait()

    def sweep0(e, into):
        finish(level0, e)
        if e == 0:
            tell_far(0)
        with jax.named_scope("sweep0"):
            ghost_ext(recv0, ext0, nb, e)
            rest = []
            if e == 0:
                rest = [(b, i) for b in range(nb - mixed, nb) for i in range(k0)]
            each = -(-len(rest) // max(nb - mixed, 1))
            for b in range(nb):
                for late, i in rest[b * each : (b + 1) * each]:
                    h, t = two_terms(blocks0[late, i].T)
                    wide0[late, i * bs : (i + 1) * bs, :bs] = h
                    wide0[late, i * bs : (i + 1) * bs, bs:] = t
                c = coupled(b, cols0, ext0, wide0, k0)
                v = x0[b]
                into[b] = v + wfull0[b] * (rhs[b] - (dfull0[b] * v + c))

    def sweep1(right, into):
        with jax.named_scope("sweep1"):
            for b in range(nb1):
                c = coupled(b, cols1, ext1, wide1, k1)
                v = x1[b]
                into[b] = v + wfull1[b] * (right[b] - (dfull1[b] * v + c))

    e0 = 0
    for _ in range(NU - 1):
        sweep0(e0, x0)
        e0 += 1
        pack(x0, send0, sends0, e0)
        start(level0, e0)
        own_ext(x0, ext0, nb)

    drain(2)

    l_late[4].wait()
    for b in range(nb):
        h, t = two_terms(pro0[b])
        down0[b * bs : (b + 1) * bs, :bs] = h
        down0[b * bs : (b + 1) * bs, bs:] = t
    l_blocks1.wait()
    for b in range(nb1):
        split_blocks(b, blocks1, wide1, k1)
    l_late[5].wait()
    for b in range(nb1):
        d = jnp.broadcast_to(diag1[b : b + 1, :], (loads, bs))
        dfull1[b] = d
        wfull1[b] = OMEGA / d

    hear_far(0)
    l_late[3].wait()

    @pl.when(solving)
    def _():
        cin[my_slot] = cinv[...]
        recva[me] = aggf[...]

    seat_start(0)
    finish(level0, e0)
    tell_far(1)
    with jax.named_scope("resid0"):
        ghost_ext(recv0, ext0, nb, e0)
        for b in range(nb):
            c = coupled(b, cols0, ext0, wide0, k0)
            r = rhs[b] - (dfull0[b] * x0[b] + c)
            parts = [jnp.where(agg0[b] == a, r, 0.0) for a in range(nb1)]
            res0[:, b * bs : (b + 1) * bs] = stacked(jnp.concatenate(parts, axis=0))
        q = folded(res0[...], down0[...])
    e0 += 1

    for b in range(nb1):
        low = b * loads
        high = (nb1 + b) * loads
        total = q[low : low + loads] + q[high : high + loads]
        b1[b] = total
        x1[b] = wfull1[b] * total
    pack(x1, send1, sends1, 0, True)
    start(level1, 0)
    own_ext(x1, ext1, nb1)
    for share in range(1, shares):
        seat_start(share)
    drain(2)
    for b in range(nb1):
        h, t = two_terms(pro1[b])
        down1[b, :, :bs] = h
        down1[b, :, bs:] = t
        h, t = two_terms(pro1[b].T)
        up1[b, :, :bs] = h
        up1[b, :, bs:] = t
    for b in range(nb1):
        twice = jnp.concatenate([down1[b], down1[b]], axis=0)

        def fold(i, carry):
            at = pl.ds(pl.multiple_of(i * bs, bs), bs)
            h, t = two_terms(folded(wide1[b, at], twice))
            folded1[b, at, :bs] = h
            folded1[b, at, bs:] = t
            return carry

        lax.fori_loop(0, k1, fold, 0, unroll=7)
    for b in range(nb):
        h, t = two_terms(pro0[b].T)
        up0[b, :, :bs] = h
        up0[b, :, bs:] = t
    e1 = 0
    for _ in range(NU - 1):
        finish(level1, e1)
        if e1 == 0:
            hear_far(1)
        ghost_ext(recv1, ext1, nb1, e1)
        sweep1(b1, x1)
        e1 += 1
        pack(x1, send1, sends1, e1, True)
        start(level1, e1)
        drain(2)
        own_ext(x1, ext1, nb1)

    @pl.when(solving)
    def _():
        for share in range(shares):
            seat_ready(share)

    base = [
        joined(stacked(b1[b] - dfull1[b] * x1[b]), down1[b], loads) for b in range(nb1)
    ]
    finish(level1, e1)
    to_solvers(aggf, recva, s_asend, 0)
    with jax.named_scope("resid1"):
        ghost_ext(recv1, ext1, nb1, e1)
        for b in range(nb1):
            c = coupled(b, cols1, ext1, folded1, k1)
            mine[b * loads : (b + 1) * loads, :] = base[b] - c

    to_solvers(mine, recvc, s_msend, 1)
    for g in range(1, g1):
        for d, (goes, there, _) in enumerate(directions):
            @pl.when(goes)
            def _():
                bulk_copy(d, g - 1, there).wait_send()
        bulk_start(g)

    for b in range(nb1):
        past1[b] = coupled(b, cols1, ext1, wide1, k1)

    @pl.when(solving)
    def _():
        recvc[me] = mine[...]

    @pl.when(solving)
    def _():
        with jax.named_scope("waitC1"):
            all_bytes(recva, n - 1, s_brecv.at[0])
            all_bytes(recvc, n - 1, s_brecv.at[1])
        index = lax.broadcasted_iota(jnp.int32, (ncb, nb1 * loads, bs), 0).astype(F32)

        def collect(d, total):
            name = recva[d]
            name = jnp.concatenate(
                [jnp.broadcast_to(name[b : b + 1], (loads, bs)) for b in range(nb1)], axis=0
            )
            return total + jnp.where(name[None] == index, recvc[d][None], 0.0)

        total = lax.fori_loop(
            0, n, collect, jnp.zeros((ncb, nb1 * loads, bs), F32), unroll=8
        )
        lhs = jnp.concatenate([stacked(total[c]) for c in range(ncb)], axis=1)
        own = folded(lhs, wide2[...])
        rows = [own[i * loads : (i + 1) * loads] for i in range(2 * nb1)]
        own = functools.reduce(lambda a, b: a + b, rows)
        for m in range(pair):
            xs[m] = own[:, m * bs : (m + 1) * bs]

        def tell(r, c):
            pltpu.make_async_remote_copy(
                src_ref=xs, dst_ref=recvx.at[my_place],
                send_sem=s_xsend.at[0], recv_sem=s_brecv.at[2],
                device_id=(r, c), device_id_type=MESH,
            ).start()

        half = n_col // 2
        for i in range(1, n_col):
            step = half + (i // 2 if i % 2 else -(i // 2))
            c = wrapped(col + step, n_col)
            for j in range(n_row):
                tell(wrapped(row + (j + 1) % n_row, n_row), c)
        for j in range(1, n_row):
            tell(wrapped(row + j, n_row), col)
        recvx[my_place] = xs[...]

    for d, (_, _, comes) in enumerate(directions):
        @pl.when(comes)
        def _():
            pltpu.make_async_copy(precv.at[d], precv.at[d], s_precv.at[d]).wait()

        for g in range(g1):
            h, t = two_terms(precv[d, g, :bs].T)
            up1[nb1 + d * g1 + g, :, :bs] = h
            up1[nb1 + d * g1 + g, :, bs:] = t

    for b in range(nb1):
        def carry_over(i, carry):
            at = pl.ds(pl.multiple_of(i * bs, bs), bs)
            block = wide1[b, at]
            twice = jnp.concatenate([block, block], axis=0)
            h, t = two_terms(folded(up1[cols1[b, i]], twice))
            lifted1[b, at, :bs] = h
            lifted1[b, at, bs:] = t
            return carry

        lax.fori_loop(0, k1, carry_over, 0, unroll=7)

    @pl.when(solving)
    def _():
        with jax.named_scope("waitC2"):
            if ns > 1:
                all_bytes(recvx, ns - 1, s_brecv.at[2])

    @pl.when(jnp.logical_not(solving))
    def _():
        with jax.named_scope("waitC2"):
            all_bytes(recvx, ns, s_brecv.at[2])

    names = [jnp.broadcast_to(aggf[b : b + 1], (loads, bs)) for b in range(nb1)]
    names += [precv[d, g, bs : bs + loads] for d in range(4) for g in range(g1)]
    names = jnp.stack(names)

    def pick(tier, pieces):
        for m in range(pair):
            for group in range(groups):
                at = ((tier * pair + m) * groups + group).astype(F32)
                block = recvx[tier * groups + group, m]
                pieces = pieces + jnp.where(names == at, block[None], 0.0)
        return pieces

    pieces = lax.fori_loop(0, n_row // pair, pick, jnp.zeros(names.shape, F32), unroll=2)
    for v in range(nb1 + 4 * g1):
        pext[v] = stacked(pieces[v])
    for b in range(nb1):
        c = past1[b] + coupled(b, cols1, pext, lifted1, k1)
        v = x1[b] + joined(pext[b], up1[b], loads)
        x1[b] = v + wfull1[b] * (b1[b] - (dfull1[b] * v + c))
    e1 += 1

    for i in range(1, NU):
        pack(x1, send1, sends1, e1, True)
        start(level1, e1)
        drain(2)
        own_ext(x1, ext1, nb1)
        finish(level1, e1)
        ghost_ext(recv1, ext1, nb1, e1)
        e1 += 1
        sweep1(b1, x1)

    own_ext(x1, ext1, nb1)
    for b in range(nb):
        x0[b] = x0[b] + joined(ext1[agg0[b]], up0[b], loads)
    for i in range(NU):
        pack(x0, send0, sends0, e0)
        start(level0, e0)
        own_ext(x0, ext0, nb)
        drain(2)
        if i == NU - 1:
            for d, (goes, there, _) in enumerate(directions):
                @pl.when(goes)
                def _():
                    bulk_copy(d, g1 - 1, there).wait_send()

            @pl.when(jnp.logical_not(solving))
            def _():
                for share in range(shares):
                    seat_copy(my_slot, share).wait_send()
                all_bytes(recva, ns, s_asend.at[0])
                all_bytes(recvc, ns, s_msend.at[0])

            @pl.when(solving)
            def _():
                all_bytes(tally, n - 1, s_xsend.at[0])
                if ns > 1:
                    all_bytes(recva, ns - 1, s_asend.at[0])
                    all_bytes(recvc, ns - 1, s_msend.at[0])

        sweep0(e0, out if i == NU - 1 else x0)
        e0 += 1

    drain(1)


def on_device(
    rhs, diag0, blocks0, cols0, sends0, pro0, agg0, diag1, blocks1, cols1, sends1, pro1, agg1, cinv
):
    n_row, n_col = lax.axis_size("row"), lax.axis_size("col")
    n = n_row * n_col
    _, _, nb, loads, bs = rhs.shape
    nb1 = diag1.shape[2]
    k0, k1 = cols0.shape[3], cols1.shape[3]
    g0, g1 = sends0.shape[3], sends1.shape[3]
    owned, ncu = cinv.shape
    reps = bs // owned
    pair = 2 if n_row % 2 == 0 else 1
    ns = (n_row // pair) * (n_col // reps)
    shares = 2 if (ncu // bs) % 2 == 0 else 1
    tall = -(-2 * loads // 16) * 16
    floats = [a[0, 0] for a in (rhs, diag0, blocks0, pro0, diag1, blocks1, pro1)] + [cinv]
    ints = [a[0, 0] for a in (cols0, sends0, agg0, cols1)]
    ints += [sends1[0, 0].T, agg1[0, 0]]
    vm = pltpu.VMEM
    dma = pltpu.SemaphoreType.DMA
    scratch = [vm(a.shape, F32) for a in floats]
    scratch += [pltpu.SMEM(a.shape, jnp.int32) for a in ints]
    scratch += [dma((6 + (nb // 2 if nb % 2 == 0 else nb),))]
    scratch += [vm((nb, k0 * bs, 2 * bs), BF16)] + [vm((nb1, k1 * bs, 2 * bs), BF16)] * 3
    scratch += [vm((nb * bs, 2 * bs), BF16), vm((nb, bs, 2 * bs), BF16)]
    scratch += [vm((nb1, bs, 2 * bs), BF16), vm((nb1 + 4 * g1, bs, 2 * bs), BF16)]
    scratch += [vm((pair * reps, owned, ncu), F32), vm((ncu, 2 * pair * bs), BF16)]
    scratch += [vm((nb, loads, bs), F32)] * 2
    scratch += [vm((nb1, loads, bs), F32)] * 2
    scratch += [vm((nb + 4 * g0, tall, bs), BF16), vm((nb1 + 4 * g1, tall, bs), BF16)]
    scratch += [vm((nb1 + 4 * g1, tall, bs), BF16)]
    scratch += [vm((nb, loads, bs), F32)] + [vm((nb1, loads, bs), F32)] * 3
    scratch += [vm((-(-2 * nb1 * loads // 16) * 16, nb * bs), BF16)]
    scratch += [vm((2 * NU, 4, g0, loads, bs), F32)] * 2
    scratch += [vm((2 * NU - 1, 4, g1, loads, bs), F32)] * 2
    scratch += [vm((4, g1, bs + 8, bs), F32)] * 2
    scratch += [vm((nb1, bs), F32), vm((n, nb1, bs), F32)]
    scratch += [vm((nb1 * loads, bs), F32), vm((n, nb1 * loads, bs), F32)]
    scratch += [vm((pair, loads, bs), F32), vm((ns, pair, loads, bs), F32)]
    scratch += [vm((n - 1, pair, loads, bs), F32)]
    scratch += [dma((2, 4))] * 2 + [dma((4,))] * 2
    scratch += [dma((shares,))] * 2 + [dma((1,))] * 3 + [dma((3,))]
    scratch += [pltpu.SemaphoreType.REGULAR((2,))]
    result = pl.pallas_call(
        functools.partial(kernel, n_row, n_col, pair),
        out_shape=pltpu.VMEM((nb, loads, bs), F32),
        in_specs=[pl.BlockSpec(memory_space=pl.ANY)] * 14,
        out_specs=pl.BlockSpec(memory_space=pltpu.VMEM),
        scratch_shapes=scratch,
        compiler_params=pltpu.CompilerParams(
            collective_id=0, has_side_effects=True, vmem_limit_bytes=60 * 1024 * 1024
        ),
    )(*ints, *floats)
    return result[None, None]


def solution(mesh):
    return jax.shard_map(
        on_device,
        mesh=mesh,
        in_specs=(
            P("row", "col", None, None, None),
            P("row", "col", None, None),
            P("row", "col", None, None, None, None),
            P("row", "col", None, None),
            P("row", "col", None, None),
            P("row", "col", None, None, None),
            P("row", "col", None),
            P("row", "col", None, None),
            P("row", "col", None, None, None, None),
            P("row", "col", None, None),
            P("row", "col", None, None),
            P("row", "col", None, None, None),
            P("row", "col", None),
            P(("row", "col"), None),
        ),
        out_specs=P("row", "col", None, None, None),
        check_vma=False,
    )
```

```python
import functools

import jax
import jax.numpy as jnp
from jax import lax
from jax.experimental import pallas as pl
from jax.experimental.pallas import tpu as pltpu
from jax.sharding import PartitionSpec as P

NU = 2
OMEGA = 0.3
F32 = jnp.float32
BF16 = jnp.bfloat16
MESH = pl.DeviceIdType.MESH
NN = (((1,), (0,)), ((), ()))


def two_terms(value):
    head = value.astype(BF16)
    tail = (value - head.astype(F32)).astype(BF16)
    return head, tail


def stacked(value):
    head = value.astype(BF16).astype(F32)
    rows = 2 * value.shape[0]
    pad = -rows % 16
    parts = [head, value - head]
    if pad:
        parts.append(jnp.zeros((pad, value.shape[1]), F32))
    return jnp.concatenate(parts, axis=0).astype(BF16)


def folded(lhs, wide):
    both = lax.dot_general(lhs, wide, NN, preferred_element_type=F32)
    half = both.shape[1] // 2
    return both[:, :half] + both[:, half:]


def joined(lhs, wide, rows):
    both = folded(lhs, wide)
    return both[:rows] + both[rows : 2 * rows]


def seat_of(group, groups, reps):
    if 2 * group + 1 < groups:
        return group * reps + reps - 1
    if 2 * group + 1 > groups:
        return group * reps
    return group * reps + reps // 2


def reaches(n_row, n_col, pair, groups, reps):
    grid = [(r, c) for r in range(n_row) for c in range(n_col)]

    def beside(p, row_steps, col_steps):
        steps = [(d, 0) for d in row_steps] + [(0, d) for d in col_steps]
        spots = [(p[0] + a, p[1] + b) for a, b in steps]
        return [q for q in spots if 0 <= q[0] < n_row and 0 <= q[1] < n_col]

    def heard(known, jump):
        told = {}
        for p in grid:
            near = beside(p, (-1, 1), (-1, 1)) + (beside(p, (), (-2, 2)) if jump else [])
            told[p] = known[p].union(*[known[q] for q in near])
        return told

    first = heard({p: {p} for p in grid}, False)
    second = heard(first, False)
    early = {}
    for r, c in grid:
        far = [(r, c + d) for d in (-2, 2) if 0 <= c + d < n_col]
        early[(r, c)] = second[(r, c)].union(*[second[q] for q in far])
    third = heard(second, True)
    last = heard(heard(third, True), False)
    seats = [seat_of(group, groups, reps) for group in range(groups)]
    for r, c in grid:
        solvers = {(t, s) for t in range(pair - 1, n_row, pair) for s in seats}
        own = (r // pair * pair + pair - 1, seats[c // reps])
        if own not in early[(r, c)] or not solvers <= last[(r, c)]:
            return False
    return True


def kernel(
    n_row, n_col, pair,
    cols0_h, sends0_h, agg0_h, cols1_h, sends1_h, agg1_h,
    rhs_h, diag0_h, blocks0_h, pro0_h, diag1_h, blocks1_h, pro1_h, cinv_h,
    out,
    rhs, diag0, blocks0, pro0, diag1, blocks1, pro1, cinv,
    cols0, sends0, agg0, cols1, sends1, agg1,
    in_sem,
    wide0, wide1, folded1, lifted1, down0, up0, down1, up1, cin, wide2,
    dfull0, wfull0, dfull1, wfull1,
    ext0, ext1, pext, x0, x1, b1, past1, res0,
    send0, recv0, send1, recv1, psend, precv,
    aggf, recva, mine, recvc, xs, recvx, tally,
    s_send, s_recv, s_psend, s_precv,
    s_cin, s_csend, s_asend, s_msend, s_xsend, s_brecv, s_far,
):
    nb, loads, bs = rhs.shape
    nb1 = diag1.shape[0]
    k0 = blocks0.shape[1]
    k1 = blocks1.shape[1]
    g1 = send1.shape[2]
    n = n_row * n_col
    owned, ncu = cinv.shape
    ncb = ncu // bs
    reps = bs // owned
    groups = n_col // reps
    ns = (n_row // pair) * groups
    row = lax.axis_index("row")
    col = lax.axis_index("col")
    me = row * n_col + col

    seats = [seat_of(group, groups, reps) for group in range(groups)]
    solvers = [
        (tier * pair + pair - 1, seats[group])
        for tier in range(n_row // pair) for group in range(groups)
    ]
    my_tier, my_group = row // pair, col // reps
    my_seat = jnp.int32(0)
    for group in range(groups):
        my_seat = jnp.where(my_group == group, seats[group], my_seat)
    solving = (lax.rem(row, pair) == pair - 1) & (col == my_seat)
    my_place = my_tier * groups + my_group
    my_slot = lax.rem(row, pair) * reps + lax.rem(col, reps)

    directions = (
        (row < n_row - 1, (row + 1, col), row > 0),
        (row > 0, (row - 1, col), row < n_row - 1),
        (col < n_col - 1, (row, col + 1), col > 0),
        (col > 0, (row, col - 1), col < n_col - 1),
    )

    def wrapped(i, size):
        return jnp.where(i >= size, i - size, i)

    barrier = pltpu.get_barrier_semaphore()
    relayed = reaches(n_row, n_col, pair, groups, reps)

    def greet(r, c):
        pl.semaphore_signal(barrier, inc=1, device_id=(r, c), device_id_type=MESH)

    loading = []

    def load(source, target):
        copy = pltpu.make_async_copy(source, target, in_sem.at[len(loading) % in_sem.shape[0]])
        loading.append(copy)
        copy.start()
        return copy

    if relayed:
        for goes, (r, c) in [(goes, there) for goes, there, _ in directions]:
            @pl.when(goes)
            def _():
                greet(r, c)
    else:
        for i in range(1, n_row):
            greet(wrapped(row + i, n_row), col)

    l_ints = [load(sends0_h, sends0), load(sends1_h, sends1), load(agg1_h, agg1)]
    l_rhs = load(rhs_h, rhs)
    l_diag0 = load(diag0_h, diag0)
    l_pro1 = load(pro1_h, pro1)
    step = 2 if nb % 2 == 0 else 1
    l_blocks0 = [
        load(blocks0_h.at[pl.ds(b, step)], blocks0.at[pl.ds(b, step)]) for b in range(0, nb, step)
    ]

    if not relayed:
        def greet_line(i, carry):
            c = wrapped(col + i, n_col)
            for r in range(n_row):
                greet(r, c)
            return carry

        lax.fori_loop(1, n_col, greet_line, 0, unroll=min(n_col - 1, 7))

    for d, (_, _, comes) in enumerate(directions):
        @pl.when(jnp.logical_not(comes))
        def _():
            for e in range(recv0.shape[0]):
                recv0[e, d] = jnp.zeros(recv0.shape[2:], F32)
            for e in range(recv1.shape[0]):
                recv1[e, d] = jnp.zeros(recv1.shape[2:], F32)
            precv[d] = jnp.zeros(precv.shape[1:], F32)

    order = []
    partners = jnp.int32(0)
    for goes, _, _ in directions:
        partners = partners + jnp.where(goes, 1, 0)

    def settle(part_of, sem):
        for k in range(1, 5):
            @pl.when(partners == k)
            def _():
                part = part_of(pl.ds(0, k))
                pltpu.make_async_copy(part, part, sem).wait()


    def halo_copy(level, e, d, there):
        send, recv = level
        turn = order.index((level is level1, e)) % 2
        return pltpu.make_async_remote_copy(
            src_ref=send.at[e, d], dst_ref=recv.at[e, d],
            send_sem=s_send.at[turn], recv_sem=s_recv.at[turn],
            device_id=there, device_id_type=MESH,
        )

    def pack(x, send, sends, e, flip=False):
        for d in range(4):
            for g in range(send.shape[2]):
                send[e, d, g] = x[sends[g, d] if flip else sends[d, g]]

    def start(level, e):
        order.append((level is level1, e))
        for d in (2, 3, 0, 1):
            goes, there, _ = directions[d]

            @pl.when(goes)
            def _():
                halo_copy(level, e, d, there).start()

    def finish(level, e):
        with jax.named_scope("finish"):
            turn = order.index((level is level1, e)) % 2
            settle(lambda some: level[1].at[e, some], s_recv.at[turn])

    def drain(back):
        if back > len(order):
            return
        upper, e = order[-back]
        recv = recv1 if upper else recv0
        settle(lambda some: recv.at[e, some], s_send.at[(len(order) - back) % 2])

    level0 = (send0, recv0)
    level1 = (send1, recv1)

    def bulk_copy(d, g, there):
        return pltpu.make_async_remote_copy(
            src_ref=psend.at[d, g], dst_ref=precv.at[d, g],
            send_sem=s_psend.at[0], recv_sem=s_precv.at[0],
            device_id=there, device_id_type=MESH,
        )

    def bulk_start(g):
        for d, (goes, there, _) in enumerate(directions):
            psend[d, g, :bs] = pro1[sends1[g, d]]
            psend[d, g, bs:] = jnp.full((8, bs), agg1[sends1[g, d]].astype(F32))

            @pl.when(goes)
            def _():
                bulk_copy(d, g, there).start()

    def own_ext(x, ext, count):
        for b in range(count):
            ext[b] = stacked(x[b])

    def ghost_ext(recv, ext, count, e):
        ghosts = recv.shape[2]
        for d in range(4):
            for g in range(ghosts):
                ext[count + d * ghosts + g] = stacked(recv[e, d, g])

    def coupled(b, cols, ext, wide, k):
        lhs = jnp.concatenate([ext[cols[b, i]] for i in range(k)], axis=1)
        return joined(lhs, wide[b], loads)

    def split_blocks(b, blocks, wide, k):
        def one(i, carry):
            h, t = two_terms(blocks[b, i].T)
            at = pl.ds(pl.multiple_of(i * bs, bs), bs)
            wide[b, at, :bs] = h
            wide[b, at, bs:] = t
            return carry

        lax.fori_loop(0, k, one, 0, unroll=7)

    def arrive(b):
        if b % step == 0:
            l_blocks0[b // step].wait()
        split_blocks(b, blocks0, wide0, k0)

    shares = s_csend.shape[0]
    width = ncu // shares

    def seat_copy(slot, share):
        lanes = pl.ds(share * width, width)
        return pltpu.make_async_remote_copy(
            src_ref=cinv.at[:, lanes], dst_ref=cin.at[slot, :, lanes],
            send_sem=s_csend.at[share], recv_sem=s_cin.at[share],
            device_id=(my_tier * pair + pair - 1, my_seat), device_id_type=MESH,
        )

    def seat_start(share):
        @pl.when(jnp.logical_not(solving))
        def _():
            seat_copy(my_slot, share).start()

    def seat_ready(share):
        if pair * reps > 1:
            part = cin.at[pl.ds(0, pair * reps - 1), :, pl.ds(share * width, width)]
            pltpu.make_async_copy(part, part, s_cin.at[share]).wait()

        def one(c, carry):
            at = pl.ds(pl.multiple_of(c * bs, bs), bs)
            for m in range(pair):
                piece = cin[m * reps : (m + 1) * reps, :, at].reshape(bs, bs)
                h, t = two_terms(piece.T)
                wide2[at, m * bs : (m + 1) * bs] = h
                wide2[at, (pair + m) * bs : (pair + m + 1) * bs] = t
            return carry

        first = share * (ncb // shares)
        lax.fori_loop(first, first + ncb // shares, one, 0, unroll=4 if ncb // shares % 4 == 0 else 1)

    l_rhs.wait()
    l_diag0.wait()
    for b in range(nb):
        d = jnp.broadcast_to(diag0[b : b + 1, :], (loads, bs))
        w = OMEGA / d
        dfull0[b] = d
        wfull0[b] = w
        x0[b] = w * rhs[b]
    for copy in l_ints:
        copy.wait()
    pack(x0, send0, sends0, 0)
    with jax.named_scope("barrier"):
        if relayed:
            count = jnp.int32(0)
            for _, _, comes in directions:
                count = count + jnp.where(comes, 1, 0)
            pl.semaphore_wait(barrier, count)
        else:
            pl.semaphore_wait(barrier, n - 1)
    start(level0, 0)
    l_pro1.wait()
    bulk_start(0)
    l_late = [
        load(source, target)
        for source, target in (
            (cols0_h, cols0), (agg0_h, agg0), (cols1_h, cols1), (cinv_h, cinv), (pro0_h, pro0),
            (diag1_h, diag1),
        )
    ]
    own_ext(x0, ext0, nb)
    for b in range(nb1):
        aggf[b : b + 1, :] = jnp.full((1, bs), agg1[b].astype(F32))
    arrive(0)
    l_blocks1 = load(blocks1_h, blocks1)
    mixed = 3
    for b in range(1, nb - mixed):
        arrive(b)
    for copy in l_late[:3]:
        copy.wait()
    if mixed:
        for b in range(nb - mixed, nb):
            if b % step == 0:
                l_blocks0[b // step].wait()

    def tell_far(jump):
        if relayed:
            for goes, c in ((col + 2 < n_col, col + 2), (col > 1, col - 2)):
                @pl.when(goes)
                def _():
                    pl.semaphore_signal(
                        s_far.at[jump], inc=1, device_id=(row, c), device_id_type=MESH
                    )

    def hear_far(jump):
        if relayed:
            count = jnp.where(col + 2 < n_col, 1, 0) + jnp.where(col > 1, 1, 0)
            pl.semaphore_wait(s_far.at[jump], count)

    def to_solvers(src, dst, s_out, which):
        for r, c in solvers:
            @pl.when((row != r) | (col != c))
            def _():
                pltpu.make_async_remote_copy(
                    src_ref=src, dst_ref=dst.at[me],
                    send_sem=s_out.at[0], recv_sem=s_brecv.at[which],
                    device_id=(r, c), device_id_type=MESH,
                ).start()

    def all_bytes(dst, count, sem):
        part = dst.at[pl.ds(0, count)]
        pltpu.make_async_copy(part, part, sem).wait()

    def sweep0(e, into):
        finish(level0, e)
        if e == 0:
            tell_far(0)
        with jax.named_scope("sweep0"):
            ghost_ext(recv0, ext0, nb, e)
            rest = []
            if e == 0:
                rest = [(b, i) for b in range(nb - mixed, nb) for i in range(k0)]
            each = -(-len(rest) // max(nb - mixed, 1))
            for b in range(nb):
                for late, i in rest[b * each : (b + 1) * each]:
                    h, t = two_terms(blocks0[late, i].T)
                    wide0[late, i * bs : (i + 1) * bs, :bs] = h
                    wide0[late, i * bs : (i + 1) * bs, bs:] = t
                c = coupled(b, cols0, ext0, wide0, k0)
                v = x0[b]
                into[b] = v + wfull0[b] * (rhs[b] - (dfull0[b] * v + c))

    def sweep1(right, into):
        with jax.named_scope("sweep1"):
            for b in range(nb1):
                c = coupled(b, cols1, ext1, wide1, k1)
                v = x1[b]
                into[b] = v + wfull1[b] * (right[b] - (dfull1[b] * v + c))

    e0 = 0
    for _ in range(NU - 1):
        sweep0(e0, x0)
        e0 += 1
        pack(x0, send0, sends0, e0)
        start(level0, e0)
        own_ext(x0, ext0, nb)

    drain(2)

    l_late[4].wait()
    for b in range(nb):
        h, t = two_terms(pro0[b])
        down0[b * bs : (b + 1) * bs, :bs] = h
        down0[b * bs : (b + 1) * bs, bs:] = t
    l_blocks1.wait()
    for b in range(nb1):
        split_blocks(b, blocks1, wide1, k1)
    l_late[5].wait()
    for b in range(nb1):
        d = jnp.broadcast_to(diag1[b : b + 1, :], (loads, bs))
        dfull1[b] = d
        wfull1[b] = OMEGA / d

    hear_far(0)
    l_late[3].wait()

    @pl.when(solving)
    def _():
        cin[my_slot] = cinv[...]
        recva[me] = aggf[...]

    seat_start(0)
    finish(level0, e0)
    tell_far(1)
    with jax.named_scope("resid0"):
        ghost_ext(recv0, ext0, nb, e0)
        for b in range(nb):
            c = coupled(b, cols0, ext0, wide0, k0)
            r = rhs[b] - (dfull0[b] * x0[b] + c)
            parts = [jnp.where(agg0[b] == a, r, 0.0) for a in range(nb1)]
            res0[:, b * bs : (b + 1) * bs] = stacked(jnp.concatenate(parts, axis=0))
        q = folded(res0[...], down0[...])
    e0 += 1

    for b in range(nb1):
        low = b * loads
        high = (nb1 + b) * loads
        total = q[low : low + loads] + q[high : high + loads]
        b1[b] = total
        x1[b] = wfull1[b] * total
    pack(x1, send1, sends1, 0, True)
    start(level1, 0)
    own_ext(x1, ext1, nb1)
    for share in range(1, shares):
        seat_start(share)
    drain(2)
    for b in range(nb1):
        h, t = two_terms(pro1[b])
        down1[b, :, :bs] = h
        down1[b, :, bs:] = t
        h, t = two_terms(pro1[b].T)
        up1[b, :, :bs] = h
        up1[b, :, bs:] = t
    for b in range(nb1):
        twice = jnp.concatenate([down1[b], down1[b]], axis=0)

        def fold(i, carry):
            at = pl.ds(pl.multiple_of(i * bs, bs), bs)
            h, t = two_terms(folded(wide1[b, at], twice))
            folded1[b, at, :bs] = h
            folded1[b, at, bs:] = t
            return carry

        lax.fori_loop(0, k1, fold, 0, unroll=7)
    for b in range(nb):
        h, t = two_terms(pro0[b].T)
        up0[b, :, :bs] = h
        up0[b, :, bs:] = t
    e1 = 0
    for _ in range(NU - 1):
        finish(level1, e1)
        if e1 == 0:
            hear_far(1)
        ghost_ext(recv1, ext1, nb1, e1)
        sweep1(b1, x1)
        e1 += 1
        pack(x1, send1, sends1, e1, True)
        start(level1, e1)
        drain(2)
        own_ext(x1, ext1, nb1)

    @pl.when(solving)
    def _():
        for share in range(shares):
            seat_ready(share)

    base = [
        joined(stacked(b1[b] - dfull1[b] * x1[b]), down1[b], loads) for b in range(nb1)
    ]
    finish(level1, e1)
    to_solvers(aggf, recva, s_asend, 0)
    with jax.named_scope("resid1"):
        ghost_ext(recv1, ext1, nb1, e1)
        for b in range(nb1):
            c = coupled(b, cols1, ext1, folded1, k1)
            mine[b * loads : (b + 1) * loads, :] = base[b] - c

    to_solvers(mine, recvc, s_msend, 1)
    for g in range(1, g1):
        settle(lambda some: precv.at[some, 0], s_psend.at[0])
        bulk_start(g)

    for b in range(nb1):
        past1[b] = coupled(b, cols1, ext1, wide1, k1)

    @pl.when(solving)
    def _():
        recvc[me] = mine[...]

    @pl.when(solving)
    def _():
        with jax.named_scope("waitC1"):
            all_bytes(recva, n - 1, s_brecv.at[0])
            all_bytes(recvc, n - 1, s_brecv.at[1])
        index = lax.broadcasted_iota(jnp.int32, (ncb, nb1 * loads, bs), 0).astype(F32)

        def collect(d, total):
            name = recva[d]
            name = jnp.concatenate(
                [jnp.broadcast_to(name[b : b + 1], (loads, bs)) for b in range(nb1)], axis=0
            )
            return total + jnp.where(name[None] == index, recvc[d][None], 0.0)

        total = lax.fori_loop(
            0, n, collect, jnp.zeros((ncb, nb1 * loads, bs), F32), unroll=8
        )
        lhs = jnp.concatenate([stacked(total[c]) for c in range(ncb)], axis=1)
        own = folded(lhs, wide2[...])
        rows = [own[i * loads : (i + 1) * loads] for i in range(2 * nb1)]
        own = functools.reduce(lambda a, b: a + b, rows)
        for m in range(pair):
            xs[m] = own[:, m * bs : (m + 1) * bs]

        def tell(r, c):
            pltpu.make_async_remote_copy(
                src_ref=xs, dst_ref=recvx.at[my_place],
                send_sem=s_xsend.at[0], recv_sem=s_brecv.at[2],
                device_id=(r, c), device_id_type=MESH,
            ).start()

        half = n_col // 2
        for i in range(1, n_col):
            step = half + (i // 2 if i % 2 else -(i // 2))
            c = wrapped(col + step, n_col)
            for j in range(n_row):
                tell(wrapped(row + (j + 1) % n_row, n_row), c)
        for j in range(1, n_row):
            tell(wrapped(row + j, n_row), col)
        recvx[my_place] = xs[...]

    settle(lambda some: precv.at[some], s_precv.at[0])
    for d in range(4):
        for g in range(g1):
            h, t = two_terms(precv[d, g, :bs].T)
            up1[nb1 + d * g1 + g, :, :bs] = h
            up1[nb1 + d * g1 + g, :, bs:] = t

    for b in range(nb1):
        def carry_over(i, carry):
            at = pl.ds(pl.multiple_of(i * bs, bs), bs)
            block = wide1[b, at]
            twice = jnp.concatenate([block, block], axis=0)
            h, t = two_terms(folded(up1[cols1[b, i]], twice))
            lifted1[b, at, :bs] = h
            lifted1[b, at, bs:] = t
            return carry

        lax.fori_loop(0, k1, carry_over, 0, unroll=7)

    @pl.when(solving)
    def _():
        with jax.named_scope("waitC2"):
            if ns > 1:
                all_bytes(recvx, ns - 1, s_brecv.at[2])

    @pl.when(jnp.logical_not(solving))
    def _():
        with jax.named_scope("waitC2"):
            all_bytes(recvx, ns, s_brecv.at[2])

    names = [jnp.broadcast_to(aggf[b : b + 1], (loads, bs)) for b in range(nb1)]
    names += [precv[d, g, bs : bs + loads] for d in range(4) for g in range(g1)]
    names = jnp.stack(names)

    def pick(tier, pieces):
        for m in range(pair):
            for group in range(groups):
                at = ((tier * pair + m) * groups + group).astype(F32)
                block = recvx[tier * groups + group, m]
                pieces = pieces + jnp.where(names == at, block[None], 0.0)
        return pieces

    pieces = lax.fori_loop(0, n_row // pair, pick, jnp.zeros(names.shape, F32), unroll=2)
    for v in range(nb1 + 4 * g1):
        pext[v] = stacked(pieces[v])
    for b in range(nb1):
        c = past1[b] + coupled(b, cols1, pext, lifted1, k1)
        v = x1[b] + joined(pext[b], up1[b], loads)
        x1[b] = v + wfull1[b] * (b1[b] - (dfull1[b] * v + c))
    e1 += 1

    for i in range(1, NU):
        pack(x1, send1, sends1, e1, True)
        start(level1, e1)
        drain(2)
        own_ext(x1, ext1, nb1)
        finish(level1, e1)
        ghost_ext(recv1, ext1, nb1, e1)
        e1 += 1
        sweep1(b1, x1)

    own_ext(x1, ext1, nb1)
    for b in range(nb):
        x0[b] = x0[b] + joined(ext1[agg0[b]], up0[b], loads)
    for i in range(NU):
        pack(x0, send0, sends0, e0)
        start(level0, e0)
        own_ext(x0, ext0, nb)
        drain(2)
        if i == NU - 1:
            settle(lambda some: precv.at[some, 0], s_psend.at[0])

            @pl.when(jnp.logical_not(solving))
            def _():
                for share in range(shares):
                    seat_copy(my_slot, share).wait_send()
                all_bytes(recva, ns, s_asend.at[0])
                all_bytes(recvc, ns, s_msend.at[0])

            @pl.when(solving)
            def _():
                all_bytes(tally, n - 1, s_xsend.at[0])
                if ns > 1:
                    all_bytes(recva, ns - 1, s_asend.at[0])
                    all_bytes(recvc, ns - 1, s_msend.at[0])

        sweep0(e0, out if i == NU - 1 else x0)
        e0 += 1

    drain(1)


def on_device(
    rhs, diag0, blocks0, cols0, sends0, pro0, agg0, diag1, blocks1, cols1, sends1, pro1, agg1, cinv
):
    n_row, n_col = lax.axis_size("row"), lax.axis_size("col")
    n = n_row * n_col
    _, _, nb, loads, bs = rhs.shape
    nb1 = diag1.shape[2]
    k0, k1 = cols0.shape[3], cols1.shape[3]
    g0, g1 = sends0.shape[3], sends1.shape[3]
    owned, ncu = cinv.shape
    reps = bs // owned
    pair = 2 if n_row % 2 == 0 else 1
    ns = (n_row // pair) * (n_col // reps)
    shares = 2 if (ncu // bs) % 2 == 0 else 1
    tall = -(-2 * loads // 16) * 16
    floats = [a[0, 0] for a in (rhs, diag0, blocks0, pro0, diag1, blocks1, pro1)] + [cinv]
    ints = [a[0, 0] for a in (cols0, sends0, agg0, cols1)]
    ints += [sends1[0, 0].T, agg1[0, 0]]
    vm = pltpu.VMEM
    dma = pltpu.SemaphoreType.DMA
    scratch = [vm(a.shape, F32) for a in floats]
    scratch += [pltpu.SMEM(a.shape, jnp.int32) for a in ints]
    scratch += [dma((6 + (nb // 2 if nb % 2 == 0 else nb),))]
    scratch += [vm((nb, k0 * bs, 2 * bs), BF16)] + [vm((nb1, k1 * bs, 2 * bs), BF16)] * 3
    scratch += [vm((nb * bs, 2 * bs), BF16), vm((nb, bs, 2 * bs), BF16)]
    scratch += [vm((nb1, bs, 2 * bs), BF16), vm((nb1 + 4 * g1, bs, 2 * bs), BF16)]
    scratch += [vm((pair * reps, owned, ncu), F32), vm((ncu, 2 * pair * bs), BF16)]
    scratch += [vm((nb, loads, bs), F32)] * 2
    scratch += [vm((nb1, loads, bs), F32)] * 2
    scratch += [vm((nb + 4 * g0, tall, bs), BF16), vm((nb1 + 4 * g1, tall, bs), BF16)]
    scratch += [vm((nb1 + 4 * g1, tall, bs), BF16)]
    scratch += [vm((nb, loads, bs), F32)] + [vm((nb1, loads, bs), F32)] * 3
    scratch += [vm((-(-2 * nb1 * loads // 16) * 16, nb * bs), BF16)]
    scratch += [vm((2 * NU, 4, g0, loads, bs), F32)] * 2
    scratch += [vm((2 * NU - 1, 4, g1, loads, bs), F32)] * 2
    scratch += [vm((4, g1, bs + 8, bs), F32)] * 2
    scratch += [vm((nb1, bs), F32), vm((n, nb1, bs), F32)]
    scratch += [vm((nb1 * loads, bs), F32), vm((n, nb1 * loads, bs), F32)]
    scratch += [vm((pair, loads, bs), F32), vm((ns, pair, loads, bs), F32)]
    scratch += [vm((n - 1, pair, loads, bs), F32)]
    scratch += [dma((2,))] * 2 + [dma((1,))] * 2
    scratch += [dma((shares,))] * 2 + [dma((1,))] * 3 + [dma((3,))]
    scratch += [pltpu.SemaphoreType.REGULAR((2,))]
    result = pl.pallas_call(
        functools.partial(kernel, n_row, n_col, pair),
        out_shape=pltpu.VMEM((nb, loads, bs), F32),
        in_specs=[pl.BlockSpec(memory_space=pl.ANY)] * 14,
        out_specs=pl.BlockSpec(memory_space=pltpu.VMEM),
        scratch_shapes=scratch,
        compiler_params=pltpu.CompilerParams(
            collective_id=0, has_side_effects=True, vmem_limit_bytes=60 * 1024 * 1024
        ),
    )(*ints, *floats)
    return result[None, None]


def solution(mesh):
    return jax.shard_map(
        on_device,
        mesh=mesh,
        in_specs=(
            P("row", "col", None, None, None),
            P("row", "col", None, None),
            P("row", "col", None, None, None, None),
            P("row", "col", None, None),
            P("row", "col", None, None),
            P("row", "col", None, None, None),
            P("row", "col", None),
            P("row", "col", None, None),
            P("row", "col", None, None, None, None),
            P("row", "col", None, None),
            P("row", "col", None, None),
            P("row", "col", None, None, None),
            P("row", "col", None),
            P(("row", "col"), None),
        ),
        out_specs=P("row", "col", None, None, None),
        check_vma=False,
    )
```
